8 devices in a mesh: rep: 1 (over z), pp: 8 (over x, y, core).
Axes of the slice: x: 2, y: 2, z: 1, core: 2. Of those that a mesh axis runs over, the one named last changes fastest.
Arguments:
- x: bfloat16 [16, 512, 512], P('rep')
- dy: bfloat16 [16, 512, 512], P('rep')
- w_gate: bfloat16 [8, 512, 1536], P('pp')
- w_up: bfloat16 [8, 512, 1536], P('pp')
- w_down: bfloat16 [8, 1536, 512], P('pp')
Outputs:
- output 1: bfloat16 [8, 512, 1536], P(('rep', 'pp'))
- output 2: bfloat16 [8, 512, 1536], P(('rep', 'pp'))
- output 3: bfloat16 [8, 1536, 512], P(('rep', 'pp'))
All inputs are finite; a program needn't handle non-finite values.
Results may differ from the reference program's by a relative error of at most 0.0277.
Values are sent between devices in bfloat16 or wider.
A program may use at most 2 GiB of HBM per device.

```python
import jax
import jax.numpy as jnp
from jax import lax

MICRO = 16
TOKENS = 512
D = 512
FF = 1536
LAYERS = 8
NAMES = ("w_gate", "w_up", "w_down")
SHAPES = {"w_gate": (LAYERS, D, FF), "w_up": (LAYERS, D, FF), "w_down": (LAYERS, FF, D)}


def bump(key, n, height):
    away = (jnp.arange(n, dtype=jnp.int32) - jax.random.randint(key, (), 0, n, jnp.int32)) % n
    return jnp.where(away < n // 8, height, 1.0)


def together(key, own, strength):
    shared = jax.random.normal(key, own.shape[1:], jnp.float32)
    return (own + strength * shared) * lax.rsqrt(1 + strength * strength)


def setup_inputs(seed: int = 0, part: int = 0) -> dict:
    kx, kdy, ka, kb, kz, kf, kh, kl, *kw = jax.random.split(jax.random.key(seed), 8 + len(NAMES))
    kx, kdy, ka, kb = (jax.random.fold_in(k, part) for k in (kx, kdy, ka, kb))
    shape = (MICRO, TOKENS, D)
    much_x, much_dy = jax.random.uniform(kz, (2,), jnp.float32, 0.0, 1.0)
    layers = 2.0 ** jax.random.uniform(kl, (LAYERS, 1, 1), jnp.float32, -1.0, 1.0)
    x = together(ka, jax.random.normal(kx, shape, jnp.float32), much_x) * bump(kf, D, 4.0)
    dy = together(kb, jax.random.normal(kdy, shape, jnp.float32), much_dy)
    drawn = {"x": x.astype(jnp.bfloat16), "dy": (dy * (MICRO * TOKENS) ** -0.5).astype(jnp.bfloat16)}
    for key, name in zip(kw, NAMES, strict=True):
        w = jax.random.normal(key, SHAPES[name], jnp.float32) * SHAPES[name][1] ** -0.5
        drawn[name] = (w * {"w_gate": 1.0, "w_up": bump(kh, FF, 4.0), "w_down": layers}[name]).astype(jnp.bfloat16)
    return drawn


def matmul(a, w):
    return jnp.dot(a, w, preferred_element_type=jnp.float32).astype(jnp.bfloat16)


def normed(h):
    wide = h.astype(jnp.float32)
    scale = lax.rsqrt(jnp.mean(wide**2, -1, keepdims=True) + 1e-6)
    return (wide * scale).astype(jnp.bfloat16)


def layer(h, w):
    a = normed(h)
    gate = jnp.dot(a, w["w_gate"], preferred_element_type=jnp.float32)
    up = jnp.dot(a, w["w_up"], preferred_element_type=jnp.float32)
    return h + matmul((jax.nn.silu(gate) * up).astype(jnp.bfloat16), w["w_down"])


def stack(weights, h):
    return lax.scan(lambda h, w: (layer(h, w), None), h, weights)[0]


def reference(x, dy, w_gate, w_up, w_down):
    weights = dict(zip(NAMES, (w_gate, w_up, w_down), strict=True))

    def take(so_far, one):
        h, by_y = one
        _, back = jax.vjp(lambda w: stack(w, h), weights)
        return jax.tree.map(lambda total, term: total + term.astype(jnp.float32), so_far, back(by_y)[0]), None

    none_yet = {name: jnp.zeros(w.shape, jnp.float32) for name, w in weights.items()}
    by_weights, _ = lax.scan(take, none_yet, (x, dy))
    return tuple(by_weights[name].astype(jnp.bfloat16) for name in NAMES)
```

```python
import functools

import jax
import jax.numpy as jnp
from jax import lax
from jax.experimental import pallas as pl
from jax.experimental.pallas import tpu as pltpu
from jax.sharding import PartitionSpec as P

f32, bf16 = jnp.float32, jnp.bfloat16
SLOTS = 3
OUTS = 4
PIECES = 4
FILL = 2
DRAIN = 2
TILE = 256


def dot(a, b):
    return jnp.dot(a, b, preferred_element_type=f32)


def dot_t(a, b):
    return lax.dot_general(a, b, (((1,), (1,)), ((), ())), preferred_element_type=f32)


def normed(h):
    wide = h.astype(f32)
    scale = lax.rsqrt(jnp.mean(wide * wide, -1, keepdims=True) + 1e-6)
    return wide, scale


def forward(h_ref, wg, wu, wd, si_ref, m_ref, hid_ref, out_ref):
    wide, scale = normed(h_ref[...])
    a = (wide * scale).astype(bf16)
    for j in range(wg.shape[1] // TILE):
        cs = pl.ds(j * TILE, TILE)
        g, u = dot(a, wg[:, cs]), dot(a, wu[:, cs])
        s = 1.0 / (1.0 + jnp.exp(-g))
        si = g * s
        si_ref[:, cs] = si
        m_ref[:, cs] = u * (s + si * (1.0 - s))
        hid_ref[:, cs] = (si * u).astype(bf16)
    if out_ref is not None:
        for j in range(wd.shape[1] // TILE):
            cs = pl.ds(j * TILE, TILE)
            out_ref[:, cs] = h_ref[:, cs] + dot(hid_ref[...], wd[:, cs]).astype(bf16)


def backward(h_ref, dy_ref, wg, wu, wd, si_ref, m_ref, dg_ref, du_ref, at_ref, gt_ref, through):
    dy = dy_ref[...]
    for j in range(wg.shape[1] // TILE):
        cs = pl.ds(j * TILE, TILE)
        dh = dot_t(dy, wd[cs, :]).astype(bf16).astype(f32)
        dg_ref[:, cs] = (dh * m_ref[:, cs]).astype(bf16)
        du_ref[:, cs] = (dh * si_ref[:, cs]).astype(bf16)
    wide, scale = normed(h_ref[...])
    at_ref[...] = (wide * scale).astype(bf16).T
    gt_ref[...] = dy.T
    if through:
        da = dot_t(dg_ref[...], wg[...]).astype(bf16) + dot_t(du_ref[...], wu[...]).astype(bf16)
        da = da.astype(f32)
        c = jnp.mean(da * wide, -1, keepdims=True) * (scale * scale)
        dy_ref[...] = dy + (scale * (da - wide * c)).astype(bf16)


def weights_term(acc, left, right):
    for j in range(right.shape[1] // TILE):
        cs = pl.ds(j * TILE, TILE)
        acc[:, cs] += dot(left[...], right[:, cs]).astype(bf16).astype(f32)


def kernel(stages, x, dy, wg_h, wu_h, wd_h, og, ou, od, si_h, m_h, hid_h,
           wg, wu, wd, acc_g, acc_u, acc_d, h_v, g_v, h_out, si_v, m_v, hid_v, dg_v, du_v, at_v, gt_v,
           w_sem, h_sem, g_sem, hs_sem, gs_sem, out_sem, in_sem, o_sem):
    me = lax.axis_index("pp")
    micro, rows = x.shape[0], x.shape[1]
    first, last = me == 0, me == stages - 1
    ahead = jnp.where(me >= stages - SLOTS, stages - me, 2 * (stages - me) - 2)
    ahead = jnp.minimum(ahead, 12)
    spill = me < stages - SLOTS

    barrier = pltpu.get_barrier_semaphore()

    for peer in range(stages - 1):
        to = lax.rem(me + peer + 1, stages)
        pl.semaphore_signal(barrier, inc=1, device_id={"pp": to}, device_id_type=pl.DeviceIdType.MESH)

    loads = [pltpu.make_async_copy(a.at[0], b, w_sem.at[i]) for i, (a, b) in enumerate(((wg_h, wg), (wu_h, wu), (wd_h, wd)))]

    def pieces(m, count, to, sem):
        size = rows // count
        for p in range(count):
            at = pl.ds(p * size, size)
            pltpu.make_async_copy(to[0].at[m, at], to[1].at[m, at], sem.at[m, p]).start()

    @pl.when(first)
    def _():
        pieces(0, FILL, (x, h_v), h_sem)

    for load in loads:
        load.start()

    @pl.when(first)
    def _():
        @pl.loop(1, micro)
        def _(m):
            pieces(m, 1, (x, h_v), h_sem)

    @pl.when(last)
    def _():
        pieces(micro - 1, DRAIN, (dy, g_v), g_sem)

        @pl.loop(0, micro - 1)
        def _(m):
            pieces(m, 1, (dy, g_v), g_sem)

    for acc in (acc_g, acc_u, acc_d):
        acc[...] = jnp.zeros_like(acc)
    for load in loads:
        load.wait()

    pl.semaphore_wait(barrier, stages - 1)

    def arrived(buf, sem, m, p, at):
        pltpu.make_async_copy(buf.at[m, at], buf.at[m, at], sem.at[m, p]).wait()

    def send_h(m, p, at):
        o = lax.rem(m, OUTS)
        return pltpu.make_async_remote_copy(
            h_out.at[o, at], h_v.at[m, at], hs_sem.at[o], h_sem.at[m, p], device_id={"pp": me + 1}, device_id_type=pl.DeviceIdType.MESH
        )

    def send_g(m, p, at):
        return pltpu.make_async_remote_copy(
            g_v.at[m, at], g_v.at[m, at], gs_sem.at[m], g_sem.at[m, p], device_id={"pp": me - 1}, device_id_type=pl.DeviceIdType.MESH
        )

    whole = pl.ds(0, rows)
    saved = ((si_v, si_h), (m_v, m_h), (hid_v, hid_h))

    def spill_out(m):
        return [pltpu.make_async_copy(v.at[0], h.at[m], out_sem.at[i]) for i, (v, h) in enumerate(saved)]

    def spill_in(m):
        slot = 1 + lax.rem(m, 2)
        return [pltpu.make_async_copy(h.at[m], v.at[slot], in_sem.at[lax.rem(m, 2), i]) for i, (v, h) in enumerate(saved)]

    def do_forward(m):
        slot = jnp.where(spill, 0, lax.rem(m, SLOTS))

        @pl.when(spill & (m > 0))
        def _():
            for copy in spill_out(m - 1):
                copy.wait()

        @pl.when((m >= OUTS) & (me < stages - 1))
        def _():
            send_h(m - OUTS, 0, whole).wait_send()

        def piece(p, count, out):
            size = rows // count
            at = pl.ds(pl.multiple_of(p * size, size), size)
            arrived(h_v, h_sem, m, p, at)
            o = h_out.at[lax.rem(m, OUTS), at] if out else None
            forward(h_v.at[m, at], wg, wu, wd, si_v.at[slot, at], m_v.at[slot, at], hid_v.at[slot, at], o)

            @pl.when(me < stages - 1)
            def _():
                send_h(m, p, at).start()

        @pl.when(m == 0)
        def _():
            pl.loop(0, FILL)(lambda p: piece(p, FILL, True))

        @pl.when((m > 0) & (me < stages - 1))
        def _():
            piece(0, 1, True)

        @pl.when((m > 0) & last)
        def _():
            piece(0, 1, False)

        @pl.when(spill)
        def _():
            for copy in spill_out(m):
                copy.start()

    def do_backward(m):
        slot = jnp.where(spill, 1 + lax.rem(m, 2), lax.rem(m, SLOTS))

        @pl.when(spill)
        def _():
            @pl.when(m == 0)
            def _():
                for copy in spill_in(0):
                    copy.start()

            for copy in spill_in(m):
                copy.wait()

            @pl.when(m + 1 < micro)
            def _():
                for copy in spill_in(m + 1):
                    copy.start()

        def piece(p, count, through):
            size = rows // count
            at = pl.ds(pl.multiple_of(p * size, size), size)
            arrived(g_v, g_sem, m, p, at)
            backward(h_v.at[m, at], g_v.at[m, at], wg, wu, wd, si_v.at[slot, at], m_v.at[slot, at],
                     dg_v.at[at], du_v.at[at], at_v.at[:, at], gt_v.at[:, at], through)
            if through:
                send_g(m, p, at).start()

        @pl.when((me > 0) & (m == micro - 1))
        def _():
            pl.loop(0, DRAIN)(lambda p: piece(p, DRAIN, True))

        @pl.when((me > 0) & (m < micro - 1))
        def _():
            piece(0, 1, True)

        @pl.when(first & (m == micro - 1))
        def _():
            pl.loop(0, DRAIN)(lambda p: piece(p, DRAIN, False))

        @pl.when(first & (m < micro - 1))
        def _():
            piece(0, 1, False)

        weights_term(acc_g, at_v, dg_v)
        weights_term(acc_u, at_v, du_v)
        weights_term(acc_d, gt_v, hid_v.at[slot])

    @pl.loop(0, micro + ahead - 1)
    def _(t):
        @pl.when(t < micro)
        def _():
            do_forward(t)

        @pl.when(spill & (t == micro))
        def _():
            for copy in spill_out(micro - 1):
                copy.wait()

        @pl.when(t >= ahead - 1)
        def _():
            do_backward(t - ahead + 1)

    wg[...] = acc_g[...].astype(bf16)
    outs = [pltpu.make_async_copy(b, a.at[0], o_sem.at[i]) for i, (a, b) in enumerate(((og, wg), (ou, wu), (od, wd)))]
    outs[0].start()
    wu[...] = acc_u[...].astype(bf16)
    outs[1].start()
    wd[...] = acc_d[...].astype(bf16).T
    outs[2].start()

    @pl.when(me < stages - 1)
    def _():
        for m in range(micro - OUTS, micro):
            send_h(m, 0, whole).wait_send()

    @pl.when(me > 0)
    def _():
        for m in range(micro):
            send_g(m, 0, whole).wait_send()

    for out in outs:
        out.wait()


def solution(mesh):
    stages = mesh.shape["pp"]

    def step(x, dy, w_gate, w_up, w_down):
        micro, rows, d = x.shape
        ff = w_gate.shape[2]
        hbm, vmem, dma = pl.BlockSpec(memory_space=pl.ANY), pltpu.VMEM, pltpu.SemaphoreType.DMA
        outs = pl.pallas_call(
            functools.partial(kernel, stages),
            out_shape=(
                jax.ShapeDtypeStruct(w_gate.shape, bf16),
                jax.ShapeDtypeStruct(w_up.shape, bf16),
                jax.ShapeDtypeStruct(w_down.shape, bf16),
                jax.ShapeDtypeStruct((micro, rows, ff), f32),
                jax.ShapeDtypeStruct((micro, rows, ff), f32),
                jax.ShapeDtypeStruct((micro, rows, ff), bf16),
            ),
            in_specs=[hbm] * 5,
            out_specs=(hbm,) * 6,
            scratch_shapes=[
                vmem((d, ff), bf16), vmem((d, ff), bf16), vmem((ff, d), bf16),
                vmem((d, ff), f32), vmem((d, ff), f32), vmem((d, ff), f32),
                vmem((micro, rows, d), bf16), vmem((micro, rows, d), bf16), vmem((OUTS, rows, d), bf16),
                vmem((SLOTS, rows, ff), f32), vmem((SLOTS, rows, ff), f32), vmem((SLOTS, rows, ff), bf16),
                vmem((rows, ff), bf16), vmem((rows, ff), bf16), vmem((d, rows), bf16), vmem((d, rows), bf16),
                dma((3,)), dma((micro, PIECES)), dma((micro, PIECES)), dma((OUTS,)), dma((micro,)), dma((3,)), dma((2, 3)), dma((3,)),
            ],
            compiler_params=pltpu.CompilerParams(collective_id=0, has_side_effects=True, vmem_limit_bytes=67043328),
        )(x, dy, w_gate, w_up, w_down)
        return outs[:3]

    return jax.shard_map(
        step,
        mesh=mesh,
        in_specs=(P("rep", None, None),) * 2 + (P("pp", None, None),) * 3,
        out_specs=(P(("rep", "pp"), None, None),) * 3,
        check_vma=False,
    )
```

```python
import functools

import jax
import jax.numpy as jnp
from jax import lax
from jax.experimental import pallas as pl
from jax.experimental.pallas import tpu as pltpu
from jax.sharding import PartitionSpec as P

f32, bf16 = jnp.float32, jnp.bfloat16
SLOTS = 3
OUTS = 4
PIECES = 2
TURN_H, VIA_H, TURN_G, VIA_G = 3, 0, 4, 7
CODES_H = (3, 5, 7, 9, 11, 13, 15, 17, 19, 21, 23, 25, 27, 29)
CODES_G = (3, 5, 7, 9, 11, 13, 15, 17, 19, 21, 23, 25, 27)
LENGTHS = [94, 80, 80, 80, 80, 80, 80, 93]
TABLE = (
    (0, 201523392, 503807936, 963472743, 374957463, 374957462, 150),
    (0, 335544320, 426082656, 426088025, 426088025, 601, 0),
    (0, 406921488, 541462928, 426087941, 426088025, 601, 0),
    (0, 26219076, 92561689, 426082656, 426088025, 601, 0),
    (17039360, 23355654, 23091222, 5396502, 426088024, 601, 0),
    (76562432, 408437136, 404099460, 76940673, 426087937, 601, 0),
    (403972416, 404096385, 404096385, 404096385, 404095329, 601, 0),
    (86067280, 339304536, 240182578, 348734356, 240330034, 503800020, 57),
)
TILE = 256


def dot(a, b):
    return jnp.dot(a, b, preferred_element_type=f32)


def dot_t(a, b):
    return lax.dot_general(a, b, (((1,), (1,)), ((), ())), preferred_element_type=f32)


def normed(h):
    wide = h.astype(f32)
    scale = lax.rsqrt(jnp.mean(wide * wide, -1, keepdims=True) + 1e-6)
    return wide, scale


def forward(h_ref, wg, wu, wd, si_ref, m_ref, hid_ref, out_ref):
    wide, scale = normed(h_ref[...])
    a = (wide * scale).astype(bf16)
    for j in range(wg.shape[1] // TILE):
        cs = pl.ds(j * TILE, TILE)
        g, u = dot(a, wg[:, cs]), dot(a, wu[:, cs])
        s = 1.0 / (1.0 + jnp.exp(-g))
        si = g * s
        si_ref[:, cs] = si
        m_ref[:, cs] = u * (s + si * (1.0 - s))
        hid_ref[:, cs] = (si * u).astype(bf16)
    if out_ref is not None:
        for j in range(wd.shape[1] // TILE):
            cs = pl.ds(j * TILE, TILE)
            out_ref[:, cs] = h_ref[:, cs] + dot(hid_ref[...], wd[:, cs]).astype(bf16)


def backward(h_ref, dy_ref, wg, wu, wd, si_ref, m_ref, dg_ref, du_ref, at_ref, gt_ref, through):
    dy = dy_ref[...]
    for j in range(wg.shape[1] // TILE):
        cs = pl.ds(j * TILE, TILE)
        dh = dot_t(dy, wd[cs, :]).astype(bf16).astype(f32)
        dg_ref[:, cs] = (dh * m_ref[:, cs]).astype(bf16)
        du_ref[:, cs] = (dh * si_ref[:, cs]).astype(bf16)
    wide, scale = normed(h_ref[...])
    at_ref[...] = (wide * scale).astype(bf16).T
    gt_ref[...] = dy.T
    if through:
        da = dot_t(dg_ref[...], wg[...]).astype(bf16) + dot_t(du_ref[...], wu[...]).astype(bf16)
        da = da.astype(f32)
        c = jnp.mean(da * wide, -1, keepdims=True) * (scale * scale)
        dy_ref[...] = dy + (scale * (da - wide * c)).astype(bf16)


def weights_term(acc, left, right):
    for j in range(right.shape[1] // TILE):
        cs = pl.ds(j * TILE, TILE)
        acc[:, cs] += dot(left[...], right[:, cs]).astype(bf16).astype(f32)


def pick(index, values):
    out = values[-1]
    for i in range(len(values) - 2, -1, -1):
        out = jnp.where(index == i, values[i], out)
    return jnp.int32(out)


def kernel(stages, x, dy, wg_h, wu_h, wd_h, og, ou, od, si_h, m_h, hid_h, relay,
           wg, wu, wd, acc_g, acc_u, acc_d, h_v, g_v, h_out, si_v, m_v, hid_v, dg_v, du_v, at_v, gt_v,
           w_sem, h_sem, g_sem, hs_sem, gs_sem, out_sem, in_sem, o_sem, rr_sem, rs_sem):
    me = lax.axis_index("pp")
    micro, rows = x.shape[0], x.shape[1]
    size = rows // PIECES
    first, last = me == 0, me == stages - 1
    spill = me < stages - 2

    barrier = pltpu.get_barrier_semaphore()
    for peer in range(stages - 1):
        to = lax.rem(me + peer + 1, stages)
        pl.semaphore_signal(barrier, inc=1, device_id={"pp": to}, device_id_type=pl.DeviceIdType.MESH)

    loads = [pltpu.make_async_copy(a.at[0], b, w_sem.at[i]) for i, (a, b) in enumerate(((wg_h, wg), (wu_h, wu), (wd_h, wd)))]

    def load_pieces(m, src, to, sem):
        for p in range(PIECES):
            at = pl.ds(p * size, size)
            pltpu.make_async_copy(src.at[m, at], to.at[m, at], sem.at[m, p]).start()

    @pl.when(first)
    def _():
        load_pieces(0, x, h_v, h_sem)

    for load in loads:
        load.start()

    @pl.when(first)
    def _():
        @pl.loop(1, micro)
        def _(m):
            load_pieces(m, x, h_v, h_sem)

    @pl.when(last)
    def _():
        @pl.loop(0, micro)
        def _(m):
            load_pieces(m, dy, g_v, g_sem)

    for acc in (acc_g, acc_u, acc_d):
        acc[...] = jnp.zeros_like(acc)
    for load in loads:
        load.wait()
    pl.semaphore_wait(barrier, stages - 1)

    def arrived(buf, sem, m, p, at):
        pltpu.make_async_copy(buf.at[m, at], buf.at[m, at], sem.at[m, p]).wait()

    def remote(src, dst, send, recv, to):
        return pltpu.make_async_remote_copy(src, dst, send, recv, device_id={"pp": to}, device_id_type=pl.DeviceIdType.MESH)

    def relayed(codes, m, p):
        return functools.reduce(jnp.logical_or, [m * PIECES + p == c for c in codes], False)

    def pass_on(src, m, p, at, send, dst, recv, to, turn, via, codes):
        detour = (me == turn) & relayed(codes, m, p) if codes else False

        @pl.when(jnp.logical_not(detour))
        def _():
            remote(src, dst.at[m, at], send, recv.at[m, p], to).start()

        if codes:
            @pl.when(detour)
            def _():
                remote(src, relay.at[m * PIECES + p], send, rr_sem.at[m * PIECES + p], via).start()

    def sent_h(m):
        o = lax.rem(m, OUTS)
        remote(h_out.at[o], h_v.at[m], hs_sem.at[o], h_sem.at[m, 0], me + 1).wait_send()

    saved = ((si_v, si_h), (m_v, m_h), (hid_v, hid_h))

    def spill_out(m, p, at):
        return [pltpu.make_async_copy(v.at[0, at], h.at[m, at], out_sem.at[p, i]) for i, (v, h) in enumerate(saved)]

    def spill_in(m):
        slot = lax.rem(m, 2)
        return [pltpu.make_async_copy(h.at[m], v.at[1 + slot], in_sem.at[slot, i]) for i, (v, h) in enumerate(saved)]

    def rows_of(p):
        return pl.ds(pl.multiple_of(p * size, size), size)

    def do_forward(n, fetched):
        m, p = lax.div(n, PIECES), lax.rem(n, PIECES)
        at = rows_of(p)
        slot = jnp.where(spill, 0, lax.rem(m, SLOTS))

        @pl.when(spill & (m > 0) & (fetched < m))
        def _():
            for copy in spill_out(m - 1, p, at):
                copy.wait()

        @pl.when((p == 0) & (m >= OUTS) & (me < stages - 1))
        def _():
            sent_h(m - OUTS)

        arrived(h_v, h_sem, m, p, at)
        keep = si_v.at[slot, at], m_v.at[slot, at], hid_v.at[slot, at]

        @pl.when(me < stages - 1)
        def _():
            o = lax.rem(m, OUTS)
            forward(h_v.at[m, at], wg, wu, wd, *keep, h_out.at[o, at])
            pass_on(h_out.at[o, at], m, p, at, hs_sem.at[o], h_v, h_sem, me + 1, TURN_H, VIA_H, CODES_H)

        @pl.when(last)
        def _():
            forward(h_v.at[m, at], wg, wu, wd, *keep, None)

        @pl.when(spill)
        def _():
            for copy in spill_out(m, p, at):
                copy.start()

    def fetch(m, forwards):
        for p in range(PIECES):
            @pl.when(forwards <= (m + 1) * PIECES + p)
            def _():
                for copy in spill_out(m, p, pl.ds(p * size, size)):
                    copy.wait()

        for copy in spill_in(m):
            copy.start()

    def do_backward(n, forwards, fetched):
        m, p = lax.div(n, PIECES), lax.rem(n, PIECES)
        at = rows_of(p)
        slot = jnp.where(spill, 1 + lax.rem(m, 2), lax.rem(m, SLOTS))

        @pl.when(spill & (p == 0))
        def _():
            @pl.when(fetched <= m)
            def _():
                fetch(m, forwards)

            for copy in spill_in(m):
                copy.wait()

            @pl.when((m + 1 < micro) & (forwards >= (m + 2) * PIECES))
            def _():
                fetch(m + 1, forwards)

        arrived(g_v, g_sem, m, p, at)

        def work(through):
            backward(h_v.at[m, at], g_v.at[m, at], wg, wu, wd, si_v.at[slot, at], m_v.at[slot, at],
                     dg_v.at[at], du_v.at[at], at_v.at[:, at], gt_v.at[:, at], through)

        @pl.when(me > 0)
        def _():
            work(True)
            pass_on(g_v.at[m, at], m, p, at, gs_sem.at[m], g_v, g_sem, me - 1, TURN_G, VIA_G, CODES_G)

        @pl.when(first)
        def _():
            work(False)

    def do_weights(m):
        slot = jnp.where(spill, 1 + lax.rem(m, 2), lax.rem(m, SLOTS))
        weights_term(acc_g, at_v, dg_v)
        weights_term(acc_u, at_v, du_v)
        weights_term(acc_d, gt_v, hid_v.at[slot])

    def do_relay(n):
        def hop(codes, dst, recv, to):
            c = pick(n, codes)
            m, p = lax.div(c, PIECES), lax.rem(c, PIECES)
            pltpu.make_async_copy(relay.at[c], relay.at[c], rr_sem.at[c]).wait()
            remote(relay.at[c], dst.at[m, rows_of(p)], rs_sem.at[c], recv.at[m, p], to).start()

        if CODES_H:
            @pl.when(me == VIA_H)
            def _():
                hop(CODES_H, h_v, h_sem, TURN_H + 1)

        if CODES_G:
            @pl.when(me == VIA_G)
            def _():
                hop(CODES_G, g_v, g_sem, TURN_G - 1)

    total = pick(me, LENGTHS)
    words = len(TABLE[0])

    def block(w, carry):
        word = pick(w, [pick(me, [row[i] for row in TABLE]) for i in range(words)])

        def turn(_, carry):
            word, nf, nb, nw, nr, fetched = carry
            op = lax.rem(word, 4)

            @pl.when(op == 0)
            def _():
                do_forward(nf, fetched)

            @pl.when(op == 1)
            def _():
                do_backward(nb, nf, fetched)

            @pl.when(op == 2)
            def _():
                do_weights(nw)

            if CODES_H or CODES_G:
                @pl.when(op == 3)
                def _():
                    do_relay(nr)

            m = lax.div(nb, PIECES)
            more = jnp.where((m + 1 < micro) & (nf >= (m + 2) * PIECES), m + 2, m + 1)
            fetched = jnp.where((op == 1) & (lax.rem(nb, PIECES) == 0), more, fetched)
            one = jnp.int32(1)
            return (lax.div(word, 4), nf + jnp.where(op == 0, one, 0), nb + jnp.where(op == 1, one, 0),
                    nw + jnp.where(op == 2, one, 0), nr + jnp.where(op == 3, one, 0), fetched)

        return lax.fori_loop(0, jnp.minimum(15, total - 15 * w), turn, (word, *carry))[1:]

    lax.fori_loop(0, lax.div(total + 14, 15), block, (jnp.int32(0),) * 5)

    wg[...] = acc_g[...].astype(bf16)
    outs = [pltpu.make_async_copy(b, a.at[0], o_sem.at[i]) for i, (a, b) in enumerate(((og, wg), (ou, wu), (od, wd)))]
    outs[0].start()
    wu[...] = acc_u[...].astype(bf16)
    outs[1].start()
    wd[...] = acc_d[...].astype(bf16).T
    outs[2].start()

    @pl.when(me < stages - 1)
    def _():
        for m in range(micro - OUTS, micro):
            sent_h(m)

    @pl.when(me > 0)
    def _():
        for m in range(micro):
            remote(g_v.at[m], g_v.at[m], gs_sem.at[m], g_sem.at[m, 0], me - 1).wait_send()

    for via, codes in ((VIA_H, CODES_H), (VIA_G, CODES_G)):
        @pl.when(me == via)
        def _():
            for c in codes:
                remote(relay.at[c], relay.at[c], rs_sem.at[c], rr_sem.at[c], TURN_H).wait_send()

    for out in outs:
        out.wait()


def solution(mesh):
    stages = mesh.shape["pp"]

    def step(x, dy, w_gate, w_up, w_down):
        micro, rows, d = x.shape
        ff = w_gate.shape[2]
        hbm, vmem, dma = pl.BlockSpec(memory_space=pl.ANY), pltpu.VMEM, pltpu.SemaphoreType.DMA
        outs = pl.pallas_call(
            functools.partial(kernel, stages),
            out_shape=(
                jax.ShapeDtypeStruct(w_gate.shape, bf16),
                jax.ShapeDtypeStruct(w_up.shape, bf16),
                jax.ShapeDtypeStruct(w_down.shape, bf16),
                jax.ShapeDtypeStruct((micro, rows, ff), f32),
                jax.ShapeDtypeStruct((micro, rows, ff), f32),
                jax.ShapeDtypeStruct((micro, rows, ff), bf16),
                jax.ShapeDtypeStruct((micro * PIECES, rows // PIECES, d), bf16),
            ),
            in_specs=[hbm] * 5,
            out_specs=(hbm,) * 7,
            scratch_shapes=[
                vmem((d, ff), bf16), vmem((d, ff), bf16), vmem((ff, d), bf16),
                vmem((d, ff), f32), vmem((d, ff), f32), vmem((d, ff), f32),
                vmem((micro, rows, d), bf16), vmem((micro, rows, d), bf16), vmem((OUTS, rows, d), bf16),
                vmem((SLOTS, rows, ff), f32), vmem((SLOTS, rows, ff), f32), vmem((SLOTS, rows, ff), bf16),
                vmem((rows, ff), bf16), vmem((rows, ff), bf16), vmem((d, rows), bf16), vmem((d, rows), bf16),
                dma((3,)), dma((micro, PIECES)), dma((micro, PIECES)), dma((OUTS,)), dma((micro,)), dma((PIECES, 3)), dma((2, 3)), dma((3,)),
                dma((micro * PIECES,)), dma((micro * PIECES,)),
            ],
            compiler_params=pltpu.CompilerParams(collective_id=0, has_side_effects=True, vmem_limit_bytes=67043328),
        )(x, dy, w_gate, w_up, w_down)
        return outs[:3]

    return jax.shard_map(
        step,
        mesh=mesh,
        in_specs=(P("rep", None, None),) * 2 + (P("pp", None, None),) * 3,
        out_specs=(P(("rep", "pp"), None, None),) * 3,
        check_vma=False,
    )
```

```python
import functools

import jax
import jax.numpy as jnp
from jax import lax
from jax.experimental import pallas as pl
from jax.experimental.pallas import tpu as pltpu
from jax.sharding import PartitionSpec as P

f32, bf16 = jnp.float32, jnp.bfloat16
SLOTS = 3
OUTS = 3
PIECES = 2
FINE = 4
TURN_H, VIA_H, TURN_G, VIA_G = 3, 0, 4, 7
CODES_H = (10, 12, 13, 14, 15, 16, 17, 18, 20, 21, 25, 30, 31)
CODES_G = (0, 2, 4, 5, 6, 8, 11, 13, 14, 16)
LENGTHS = [97, 84, 84, 84, 84, 84, 84, 94]
TABLE = (
    (0, 1069547520, 31328223, 629241878, 426108773, 426088025, 9561),
    (0, 155189248, 423772564, 374957441, 374957462, 152982, 0),
    (0, 84415488, 92364888, 374886994, 374957462, 152982, 0),
    (0, 542146880, 542643792, 370447889, 374957462, 152982, 0),
    (17825792, 345374994, 157287808, 101810533, 374887001, 152982, 0),
    (38010880, 92280337, 402743318, 287578201, 370447894, 152982, 0),
    (557876480, 559945236, 21501460, 23091222, 425744406, 152961, 0),
    (403973376, 21894279, 314914934, 24646797, 283479134, 278144265, 149),
)
TILE = 256


def dot(a, b):
    return jnp.dot(a, b, preferred_element_type=f32)


def normed(h):
    wide = h.astype(f32)
    scale = lax.rsqrt(jnp.mean(wide * wide, -1, keepdims=True) + 1e-6)
    return wide, scale


def forward(h_ref, wg, wu, wd, si_ref, m_ref, hid_ref, out_ref):
    wide, scale = normed(h_ref[...])
    a = (wide * scale).astype(bf16)
    for j in range(wg.shape[1] // TILE):
        cs = pl.ds(j * TILE, TILE)
        g, u = dot(a, wg[:, cs]), dot(a, wu[:, cs])
        s = 1.0 / (1.0 + jnp.exp(-g))
        si = g * s
        si_ref[:, cs] = si
        m_ref[:, cs] = u * (s + si * (1.0 - s))
        hid_ref[:, cs] = (si * u).astype(bf16)
    if out_ref is not None:
        for j in range(wd.shape[1] // TILE):
            cs = pl.ds(j * TILE, TILE)
            out_ref[:, cs] = h_ref[:, cs] + dot(hid_ref[...], wd[:, cs]).astype(bf16)


def backward(h_ref, dy_ref, wgt, wut, wdt, si_ref, m_ref, dg_ref, du_ref, at_ref, gt_ref, through):
    dy = dy_ref[...]
    for j in range(wdt.shape[1] // TILE):
        cs = pl.ds(j * TILE, TILE)
        dh = dot(dy, wdt[:, cs]).astype(bf16).astype(f32)
        dg_ref[:, cs] = (dh * m_ref[:, cs]).astype(bf16)
        du_ref[:, cs] = (dh * si_ref[:, cs]).astype(bf16)
    wide, scale = normed(h_ref[...])
    at_ref[...] = (wide * scale).astype(bf16).T
    gt_ref[...] = dy.T
    if through:
        da = dot(dg_ref[...], wgt[...]).astype(bf16) + dot(du_ref[...], wut[...]).astype(bf16)
        da = da.astype(f32)
        c = jnp.mean(da * wide, -1, keepdims=True) * (scale * scale)
        dy_ref[...] = dy + (scale * (da - wide * c)).astype(bf16)


def weights_term(acc, left, right):
    for j in range(right.shape[1] // TILE):
        cs = pl.ds(j * TILE, TILE)
        acc[:, cs] += dot(left[...], right[:, cs]).astype(bf16).astype(f32)


def pick(index, values):
    out = values[-1]
    for i in range(len(values) - 2, -1, -1):
        out = jnp.where(index == i, values[i], out)
    return jnp.int32(out)


def kernel(stages, x, dy, wg_h, wu_h, wd_h, og, ou, od, si_h, m_h, hid_h, relay,
           wg, wu, wd, wgt, wut, wdt, acc_g, acc_u, acc_d, h_v, g_v, h_out, si_v, m_v, hid_v, dg_v, du_v, at_v, gt_v,
           w_sem, h_sem, g_sem, hs_sem, gs_sem, out_sem, in_sem, o_sem, rr_sem, rs_sem):
    me = lax.axis_index("pp")
    micro, rows = x.shape[0], x.shape[1]
    size = rows // PIECES
    first, last = me == 0, me == stages - 1
    spill = me < stages - 2

    barrier = pltpu.get_barrier_semaphore()
    for peer in range(stages - 1):
        to = lax.rem(me + peer + 1, stages)
        pl.semaphore_signal(barrier, inc=1, device_id={"pp": to}, device_id_type=pl.DeviceIdType.MESH)

    loads = [pltpu.make_async_copy(a.at[0], b, w_sem.at[i]) for i, (a, b) in enumerate(((wg_h, wg), (wu_h, wu), (wd_h, wd)))]

    def load_pieces(m, src, to, sem, count=PIECES):
        for p in range(count):
            at = pl.ds(p * (rows // count), rows // count)
            pltpu.make_async_copy(src.at[m, at], to.at[m, at], sem.at[m, p]).start()

    @pl.when(first)
    def _():
        load_pieces(0, x, h_v, h_sem, FINE)

    for load in loads:
        load.start()

    @pl.when(first)
    def _():
        @pl.loop(1, micro)
        def _(m):
            load_pieces(m, x, h_v, h_sem)

    @pl.when(last)
    def _():
        @pl.loop(0, micro - 1)
        def _(m):
            load_pieces(m, dy, g_v, g_sem)

        load_pieces(micro - 1, dy, g_v, g_sem, FINE)

    for acc in (acc_g, acc_u, acc_d):
        acc[...] = jnp.zeros_like(acc)
    for load in loads:
        load.wait()
    pl.semaphore_wait(barrier, stages - 1)

    @pl.when(me > 0)
    def _():
        wgt[...] = wg[...].T
        wut[...] = wu[...].T
        wdt[...] = wd[...].T

    def arrived(buf, sem, m, p, at):
        pltpu.make_async_copy(buf.at[m, at], buf.at[m, at], sem.at[m, p]).wait()

    def remote(src, dst, send, recv, to):
        return pltpu.make_async_remote_copy(src, dst, send, recv, device_id={"pp": to}, device_id_type=pl.DeviceIdType.MESH)

    def relayed(codes, m, p):
        return functools.reduce(jnp.logical_or, [m * PIECES + p == c for c in codes], False)

    def pass_on(src, m, p, at, send, dst, recv, to, turn, via, codes):
        detour = (me == turn) & relayed(codes, m, p) if codes else False

        @pl.when(jnp.logical_not(detour))
        def _():
            remote(src, dst.at[m, at], send, recv.at[m, p], to).start()

        if codes:
            @pl.when(detour)
            def _():
                remote(src, relay.at[m * PIECES + p], send, rr_sem.at[m * PIECES + p], via).start()

    def sent_h(m):
        o = lax.rem(m, OUTS)
        remote(h_out.at[o], h_v.at[m], hs_sem.at[o], h_sem.at[m, 0], me + 1).wait_send()

    saved = ((si_v, si_h), (m_v, m_h), (hid_v, hid_h))

    def spill_out(m, p, at):
        return [pltpu.make_async_copy(v.at[0, at], h.at[m, at], out_sem.at[p, i]) for i, (v, h) in enumerate(saved)]

    def spill_in(m):
        slot = lax.rem(m, 2)
        return [pltpu.make_async_copy(h.at[m], v.at[1 + slot], in_sem.at[slot, i]) for i, (v, h) in enumerate(saved)]

    def rows_of(p, size=size):
        return pl.ds(pl.multiple_of(p * size, size), size)

    extra = FINE - PIECES

    def do_forward(n, fetched):
        fine = n < FINE
        m = jnp.where(fine, 0, lax.div(n - extra, PIECES))
        p = jnp.where(fine, n, lax.rem(n + PIECES - extra, PIECES))
        slot = jnp.where(spill, 0, lax.rem(m, SLOTS))
        o = lax.rem(m, OUTS)

        @pl.when(spill & (m > 0) & (fetched < m))
        def _():
            for copy in spill_out(m - 1, p, rows_of(p)):
                copy.wait()

        @pl.when((p == 0) & (m >= OUTS) & (me < stages - 1))
        def _():
            sent_h(m - OUTS)

        def work(size, codes):
            at = rows_of(p, size)
            arrived(h_v, h_sem, m, p, at)
            keep = si_v.at[slot, at], m_v.at[slot, at], hid_v.at[slot, at]

            @pl.when(me < stages - 1)
            def _():
                forward(h_v.at[m, at], wg, wu, wd, *keep, h_out.at[o, at])
                pass_on(h_out.at[o, at], m, p, at, hs_sem.at[o], h_v, h_sem, me + 1, TURN_H, VIA_H, codes)

            @pl.when(last)
            def _():
                forward(h_v.at[m, at], wg, wu, wd, *keep, None)

        @pl.when(fine)
        def _():
            work(rows // FINE, ())

        @pl.when(jnp.logical_not(fine))
        def _():
            work(size, CODES_H)

        finer = FINE // PIECES

        @pl.when(spill & fine & (lax.rem(n, finer) == finer - 1))
        def _():
            for copy in spill_out(0, lax.div(n, finer), rows_of(lax.div(n, finer))):
                copy.start()

        @pl.when(spill & jnp.logical_not(fine))
        def _():
            for copy in spill_out(m, p, rows_of(p)):
                copy.start()

    def fetch(m, forwards):
        for p in range(PIECES):
            @pl.when(forwards <= (m + 1) * PIECES + extra + p)
            def _():
                for copy in spill_out(m, p, pl.ds(p * size, size)):
                    copy.wait()

        for copy in spill_in(m):
            copy.start()

    def do_backward(n, forwards, fetched):
        m = jnp.minimum(lax.div(n, PIECES), micro - 1)
        p = n - m * PIECES
        fine = m == micro - 1
        slot = jnp.where(spill, 1 + lax.rem(m, 2), lax.rem(m, SLOTS))

        @pl.when(first & (n == 0))
        def _():
            wdt[...] = wd[...].T

        @pl.when(spill & (p == 0))
        def _():
            @pl.when(fetched <= m)
            def _():
                fetch(m, forwards)

            for copy in spill_in(m):
                copy.wait()

            @pl.when((m + 1 < micro) & (forwards >= (m + 2) * PIECES + extra))
            def _():
                fetch(m + 1, forwards)

        def work(size, codes):
            at = rows_of(p, size)
            arrived(g_v, g_sem, m, p, at)

            def piece(through):
                backward(h_v.at[m, at], g_v.at[m, at], wgt, wut, wdt, si_v.at[slot, at], m_v.at[slot, at],
                         dg_v.at[at], du_v.at[at], at_v.at[:, at], gt_v.at[:, at], through)

            @pl.when(me > 0)
            def _():
                piece(True)
                pass_on(g_v.at[m, at], m, p, at, gs_sem.at[m], g_v, g_sem, me - 1, TURN_G, VIA_G, codes)

            @pl.when(first)
            def _():
                piece(False)

        @pl.when(fine)
        def _():
            work(rows // FINE, ())

        @pl.when(jnp.logical_not(fine))
        def _():
            work(size, CODES_G)

    def do_weights(m):
        slot = jnp.where(spill, 1 + lax.rem(m, 2), lax.rem(m, SLOTS))
        weights_term(acc_g, at_v, dg_v)
        weights_term(acc_u, at_v, du_v)
        weights_term(acc_d, gt_v, hid_v.at[slot])

    def do_relay(n):
        def hop(codes, dst, recv, to):
            c = pick(n, codes)
            m, p = lax.div(c, PIECES), lax.rem(c, PIECES)
            pltpu.make_async_copy(relay.at[c], relay.at[c], rr_sem.at[c]).wait()
            remote(relay.at[c], dst.at[m, rows_of(p)], rs_sem.at[c], recv.at[m, p], to).start()

        if CODES_H:
            @pl.when(me == VIA_H)
            def _():
                hop(CODES_H, h_v, h_sem, TURN_H + 1)

        if CODES_G:
            @pl.when(me == VIA_G)
            def _():
                hop(CODES_G, g_v, g_sem, TURN_G - 1)

    total = pick(me, LENGTHS)
    words = len(TABLE[0])

    def block(w, carry):
        word = pick(w, [pick(me, [row[i] for row in TABLE]) for i in range(words)])

        def turn(_, carry):
            word, nf, nb, nw, nr, fetched = carry
            op = lax.rem(word, 4)

            @pl.when(op == 0)
            def _():
                do_forward(nf, fetched)

            @pl.when(op == 1)
            def _():
                do_backward(nb, nf, fetched)

            @pl.when(op == 2)
            def _():
                do_weights(nw)

            if CODES_H or CODES_G:
                @pl.when(op == 3)
                def _():
                    do_relay(nr)

            m = jnp.minimum(lax.div(nb, PIECES), micro - 1)
            more = jnp.where((m + 1 < micro) & (nf >= (m + 2) * PIECES + extra), m + 2, m + 1)
            fetched = jnp.where((op == 1) & (nb == m * PIECES), more, fetched)
            one = jnp.int32(1)
            return (lax.div(word, 4), nf + jnp.where(op == 0, one, 0), nb + jnp.where(op == 1, one, 0),
                    nw + jnp.where(op == 2, one, 0), nr + jnp.where(op == 3, one, 0), fetched)

        return lax.fori_loop(0, jnp.minimum(15, total - 15 * w), turn, (word, *carry))[1:]

    lax.fori_loop(0, lax.div(total + 14, 15), block, (jnp.int32(0),) * 5)

    wg[...] = acc_g[...].astype(bf16)
    outs = [pltpu.make_async_copy(b, a.at[0], o_sem.at[i]) for i, (a, b) in enumerate(((og, wg), (ou, wu), (od, wd)))]
    outs[0].start()
    wu[...] = acc_u[...].astype(bf16)
    outs[1].start()
    wd[...] = acc_d[...].astype(bf16).T
    outs[2].start()

    @pl.when(me < stages - 1)
    def _():
        for m in range(micro - OUTS, micro):
            sent_h(m)

    @pl.when(me > 0)
    def _():
        for m in range(micro):
            remote(g_v.at[m], g_v.at[m], gs_sem.at[m], g_sem.at[m, 0], me - 1).wait_send()

    for via, codes in ((VIA_H, CODES_H), (VIA_G, CODES_G)):
        @pl.when(me == via)
        def _():
            for c in codes:
                remote(relay.at[c], relay.at[c], rs_sem.at[c], rr_sem.at[c], TURN_H).wait_send()

    for out in outs:
        out.wait()


def solution(mesh):
    stages = mesh.shape["pp"]

    def step(x, dy, w_gate, w_up, w_down):
        micro, rows, d = x.shape
        ff = w_gate.shape[2]
        hbm, vmem, dma = pl.BlockSpec(memory_space=pl.ANY), pltpu.VMEM, pltpu.SemaphoreType.DMA
        outs = pl.pallas_call(
            functools.partial(kernel, stages),
            out_shape=(
                jax.ShapeDtypeStruct(w_gate.shape, bf16),
                jax.ShapeDtypeStruct(w_up.shape, bf16),
                jax.ShapeDtypeStruct(w_down.shape, bf16),
                jax.ShapeDtypeStruct((micro, rows, ff), f32),
                jax.ShapeDtypeStruct((micro, rows, ff), f32),
                jax.ShapeDtypeStruct((micro, rows, ff), bf16),
                jax.ShapeDtypeStruct((micro * PIECES, rows // PIECES, d), bf16),
            ),
            in_specs=[hbm] * 5,
            out_specs=(hbm,) * 7,
            scratch_shapes=[
                vmem((d, ff), bf16), vmem((d, ff), bf16), vmem((ff, d), bf16),
                vmem((ff, d), bf16), vmem((ff, d), bf16), vmem((d, ff), bf16),
                vmem((d, ff), f32), vmem((d, ff), f32), vmem((d, ff), f32),
                vmem((micro, rows, d), bf16), vmem((micro, rows, d), bf16), vmem((OUTS, rows, d), bf16),
                vmem((SLOTS, rows, ff), f32), vmem((SLOTS, rows, ff), f32), vmem((SLOTS, rows, ff), bf16),
                vmem((rows, ff), bf16), vmem((rows, ff), bf16), vmem((d, rows), bf16), vmem((d, rows), bf16),
                dma((3,)), dma((micro, FINE)), dma((micro, FINE)), dma((OUTS,)), dma((micro,)), dma((PIECES, 3)), dma((2, 3)), dma((3,)),
                dma((micro * PIECES,)), dma((micro * PIECES,)),
            ],
            compiler_params=pltpu.CompilerParams(collective_id=0, has_side_effects=True, vmem_limit_bytes=67043328),
        )(x, dy, w_gate, w_up, w_down)
        return outs[:3]

    return jax.shard_map(
        step,
        mesh=mesh,
        in_specs=(P("rep", None, None),) * 2 + (P("pp", None, None),) * 3,
        out_specs=(P(("rep", "pp"), None, None),) * 3,
        check_vma=False,
    )
```

```python
import functools

import jax
import jax.numpy as jnp
from jax import lax
from jax.experimental import pallas as pl
from jax.experimental.pallas import tpu as pltpu
from jax.sharding import PartitionSpec as P

f32, bf16 = jnp.float32, jnp.bfloat16
SLOTS = 3
OUTS = 3
PIECES = 2
FINE = 4
EARLY, LATE = 3, 3
TURN_H, VIA_H, TURN_G, VIA_G = 3, 0, 4, 7
CODES_H = (8, 9, 10, 11, 13, 17, 18, 20, 21, 23, 24, 25, 28, 30, 31)
CODES_G = (0, 3, 5, 6, 10, 14, 15, 17)
LENGTHS = [107, 92, 92, 92, 92, 92, 92, 100]
TABLE = (
    (0, 0, 98621439, 31327724, 395730523, 426088030, 362112345, 9),
    (0, 0, 307270693, 426083428, 426088025, 362112345, 9, 0),
    (0, 100990976, 140001668, 102110341, 426088025, 362112345, 9, 0),
    (0, 274808832, 369435654, 293962080, 426088006, 362112345, 9, 0),
    (268435456, 92291460, 23091288, 5788248, 307779606, 362112345, 9, 0),
    (335544320, 541139992, 404100613, 101815812, 370541956, 362112326, 9, 0),
    (537198592, 38806917, 542246277, 139986309, 542639493, 361060437, 9, 0),
    (23069952, 940892512, 87610405, 344318034, 561125296, 369448980, 611461, 0),
)
TILE = 256


def dot(a, b):
    return jnp.dot(a, b, preferred_element_type=f32)


def normed(h):
    wide = h.astype(f32)
    scale = lax.rsqrt(jnp.mean(wide * wide, -1, keepdims=True) + 1e-6)
    return wide, scale


def forward(h_ref, wg, wu, wd, si_ref, m_ref, hid_ref, out_ref):
    wide, scale = normed(h_ref[...])
    a = (wide * scale).astype(bf16)
    for j in range(wg.shape[1] // TILE):
        cs = pl.ds(j * TILE, TILE)
        g, u = dot(a, wg[:, cs]), dot(a, wu[:, cs])
        s = 1.0 / (1.0 + jnp.exp(-g))
        si = g * s
        si_ref[:, cs] = si
        m_ref[:, cs] = u * (s + si * (1.0 - s))
        hid_ref[:, cs] = (si * u).astype(bf16)
    if out_ref is not None:
        for j in range(wd.shape[1] // TILE):
            cs = pl.ds(j * TILE, TILE)
            out_ref[:, cs] = h_ref[:, cs] + dot(hid_ref[...], wd[:, cs]).astype(bf16)


def backward(h_ref, dy_ref, wgt, wut, wdt, si_ref, m_ref, dg_ref, du_ref, at_ref, gt_ref, through):
    dy = dy_ref[...]
    for j in range(wdt.shape[1] // TILE):
        cs = pl.ds(j * TILE, TILE)
        dh = dot(dy, wdt[:, cs]).astype(bf16).astype(f32)
        dg_ref[:, cs] = (dh * m_ref[:, cs]).astype(bf16)
        du_ref[:, cs] = (dh * si_ref[:, cs]).astype(bf16)
    wide, scale = normed(h_ref[...])
    at_ref[...] = (wide * scale).astype(bf16).T
    gt_ref[...] = dy.T
    if through:
        da = dot(dg_ref[...], wgt[...]).astype(bf16) + dot(du_ref[...], wut[...]).astype(bf16)
        da = da.astype(f32)
        c = jnp.mean(da * wide, -1, keepdims=True) * (scale * scale)
        dy_ref[...] = dy + (scale * (da - wide * c)).astype(bf16)


def weights_term(acc, left, right):
    for j in range(right.shape[1] // TILE):
        cs = pl.ds(j * TILE, TILE)
        acc[:, cs] += dot(left[...], right[:, cs]).astype(bf16).astype(f32)


def pick(index, values):
    out = values[-1]
    for i in range(len(values) - 2, -1, -1):
        out = jnp.where(index == i, values[i], out)
    return jnp.int32(out)


def kernel(stages, x, dy, wg_h, wu_h, wd_h, og, ou, od, si_h, m_h, hid_h, relay,
           wg, wu, wd, wgt, wut, wdt, acc_g, acc_u, acc_d, h_v, g_v, h_out, si_v, m_v, hid_v, dg_v, du_v, at_v, gt_v,
           w_sem, h_sem, g_sem, hs_sem, gs_sem, out_sem, in_sem, o_sem, rr_sem, rs_sem):
    me = lax.axis_index("pp")
    micro, rows = x.shape[0], x.shape[1]
    size = rows // PIECES
    first, last = me == 0, me == stages - 1
    spill = me < stages - 2

    barrier = pltpu.get_barrier_semaphore()
    for peer in range(stages - 1):
        to = lax.rem(me + peer + 1, stages)
        pl.semaphore_signal(barrier, inc=1, device_id={"pp": to}, device_id_type=pl.DeviceIdType.MESH)

    loads = [pltpu.make_async_copy(a.at[0], b, w_sem.at[i]) for i, (a, b) in enumerate(((wg_h, wg), (wu_h, wu), (wd_h, wd)))]

    def load_pieces(m, src, to, sem, count=PIECES):
        for p in range(count):
            at = pl.ds(p * (rows // count), rows // count)
            pltpu.make_async_copy(src.at[m, at], to.at[m, at], sem.at[m, p]).start()

    @pl.when(first)
    def _():
        load_pieces(0, x, h_v, h_sem, FINE)

    for load in loads:
        load.start()

    @pl.when(first)
    def _():
        for m in range(1, EARLY):
            load_pieces(m, x, h_v, h_sem, FINE)

        @pl.loop(EARLY, micro)
        def _(m):
            load_pieces(m, x, h_v, h_sem)

    @pl.when(last)
    def _():
        @pl.loop(0, micro - LATE)
        def _(m):
            load_pieces(m, dy, g_v, g_sem)

        for m in range(micro - LATE, micro):
            load_pieces(m, dy, g_v, g_sem, FINE)

    for acc in (acc_g, acc_u, acc_d):
        acc[...] = jnp.zeros_like(acc)
    for load in loads:
        load.wait()
    pl.semaphore_wait(barrier, stages - 1)

    @pl.when(me > 0)
    def _():
        wgt[...] = wg[...].T
        wut[...] = wu[...].T
        wdt[...] = wd[...].T

    def arrived(buf, sem, m, p, at):
        pltpu.make_async_copy(buf.at[m, at], buf.at[m, at], sem.at[m, p]).wait()

    def remote(src, dst, send, recv, to):
        return pltpu.make_async_remote_copy(src, dst, send, recv, device_id={"pp": to}, device_id_type=pl.DeviceIdType.MESH)

    def relayed(codes, m, p):
        low, high = (sum(1 << c % 16 for c in codes if c // 16 == part) for part in range(2))
        code = m * PIECES + p
        word = jnp.where(code < 16, low, high)
        return lax.rem(lax.shift_right_logical(jnp.int32(word), lax.rem(code, 16)), 2) == 1

    def pass_on(src, m, p, at, send, dst, recv, to, turn, via, codes):
        detour = (me == turn) & relayed(codes, m, p) if codes else False

        @pl.when(jnp.logical_not(detour))
        def _():
            remote(src, dst.at[m, at], send, recv.at[m, p], to).start()

        if codes:
            @pl.when(detour)
            def _():
                remote(src, relay.at[m * PIECES + p], send, rr_sem.at[m * PIECES + p], via).start()

    def sent_h(m):
        o = lax.rem(m, OUTS)
        remote(h_out.at[o], h_v.at[m], hs_sem.at[o], h_sem.at[m, 0], me + 1).wait_send()

    saved = ((si_v, si_h), (m_v, m_h), (hid_v, hid_h))

    def spill_out(m, p, at):
        return [pltpu.make_async_copy(v.at[0, at], h.at[m, at], out_sem.at[p, i]) for i, (v, h) in enumerate(saved)]

    def spill_in(m):
        slot = lax.rem(m, 2)
        return [pltpu.make_async_copy(h.at[m], v.at[1 + slot], in_sem.at[slot, i]) for i, (v, h) in enumerate(saved)]

    def rows_of(p, size=size):
        return pl.ds(pl.multiple_of(p * size, size), size)

    finer = FINE // PIECES

    def steps_before(m):
        return m * PIECES + jnp.minimum(m, EARLY) * (FINE - PIECES)

    def do_forward(n, fetched):
        fine = n < FINE * EARLY
        coarse = jnp.maximum(n - FINE * EARLY, 0)
        m = jnp.where(fine, lax.div(n, FINE), EARLY + lax.div(coarse, PIECES))
        p = jnp.where(fine, lax.rem(n, FINE), lax.rem(coarse, PIECES))
        half = jnp.where(fine, lax.div(p, finer), p)
        opens = jnp.logical_not(fine) | (lax.rem(p, finer) == 0)
        closes = jnp.logical_not(fine) | (lax.rem(p, finer) == finer - 1)
        slot = jnp.where(spill, 0, lax.rem(m, SLOTS))
        o = lax.rem(m, OUTS)

        @pl.when(spill & opens & (m > 0) & (fetched < m))
        def _():
            for copy in spill_out(m - 1, half, rows_of(half)):
                copy.wait()

        @pl.when((p == 0) & (m >= OUTS) & (me < stages - 1))
        def _():
            sent_h(m - OUTS)

        def work(size, codes):
            at = rows_of(p, size)
            arrived(h_v, h_sem, m, p, at)
            keep = si_v.at[slot, at], m_v.at[slot, at], hid_v.at[slot, at]

            @pl.when(me < stages - 1)
            def _():
                forward(h_v.at[m, at], wg, wu, wd, *keep, h_out.at[o, at])
                pass_on(h_out.at[o, at], m, p, at, hs_sem.at[o], h_v, h_sem, me + 1, TURN_H, VIA_H, codes)

            @pl.when(last)
            def _():
                forward(h_v.at[m, at], wg, wu, wd, *keep, None)

        @pl.when(fine)
        def _():
            work(rows // FINE, ())

        @pl.when(jnp.logical_not(fine))
        def _():
            work(size, CODES_H)

        @pl.when(spill & closes)
        def _():
            for copy in spill_out(m, half, rows_of(half)):
                copy.start()

    def fetch(m, forwards):
        for p in range(PIECES):
            @pl.when(forwards <= steps_before(m + 1) + p * jnp.where(m + 1 < EARLY, finer, 1))
            def _():
                for copy in spill_out(m, p, pl.ds(p * size, size)):
                    copy.wait()

        for copy in spill_in(m):
            copy.start()

    def do_backward(n, forwards, fetched):
        fine = n >= (micro - LATE) * PIECES
        late = jnp.maximum(n - (micro - LATE) * PIECES, 0)
        m = jnp.where(fine, micro - LATE + lax.div(late, FINE), lax.div(n, PIECES))
        p = jnp.where(fine, lax.rem(late, FINE), lax.rem(n, PIECES))
        slot = jnp.where(spill, 1 + lax.rem(m, 2), lax.rem(m, SLOTS))

        @pl.when(first & (n == 0))
        def _():
            wdt[...] = wd[...].T

        @pl.when(spill & (p == 0))
        def _():
            @pl.when(fetched <= m)
            def _():
                fetch(m, forwards)

            for copy in spill_in(m):
                copy.wait()

            @pl.when((m + 1 < micro) & (forwards >= steps_before(m + 2)))
            def _():
                fetch(m + 1, forwards)

        def work(size, codes):
            at = rows_of(p, size)
            arrived(g_v, g_sem, m, p, at)

            def piece(through):
                backward(h_v.at[m, at], g_v.at[m, at], wgt, wut, wdt, si_v.at[slot, at], m_v.at[slot, at],
                         dg_v.at[at], du_v.at[at], at_v.at[:, at], gt_v.at[:, at], through)

            @pl.when(me > 0)
            def _():
                piece(True)
                pass_on(g_v.at[m, at], m, p, at, gs_sem.at[m], g_v, g_sem, me - 1, TURN_G, VIA_G, codes)

            @pl.when(first)
            def _():
                piece(False)

        @pl.when(fine)
        def _():
            work(rows // FINE, ())

        @pl.when(jnp.logical_not(fine))
        def _():
            work(size, CODES_G)

    def do_weights(m):
        slot = jnp.where(spill, 1 + lax.rem(m, 2), lax.rem(m, SLOTS))
        weights_term(acc_g, at_v, dg_v)
        weights_term(acc_u, at_v, du_v)
        weights_term(acc_d, gt_v, hid_v.at[slot])

    def do_relay(n):
        def hop(codes, dst, recv, to):
            c = pick(n, codes)
            m, p = lax.div(c, PIECES), lax.rem(c, PIECES)
            pltpu.make_async_copy(relay.at[c], relay.at[c], rr_sem.at[c]).wait()
            remote(relay.at[c], dst.at[m, rows_of(p)], rs_sem.at[c], recv.at[m, p], to).start()

        if CODES_H:
            @pl.when(me == VIA_H)
            def _():
                hop(CODES_H, h_v, h_sem, TURN_H + 1)

        if CODES_G:
            @pl.when(me == VIA_G)
            def _():
                hop(CODES_G, g_v, g_sem, TURN_G - 1)

    total = pick(me, LENGTHS)
    words = len(TABLE[0])

    def block(w, carry):
        word = pick(w, [pick(me, [row[i] for row in TABLE]) for i in range(words)])

        def turn(_, carry):
            word, nf, nb, nw, nr, fetched = carry
            op = lax.rem(word, 4)

            @pl.when(op == 0)
            def _():
                do_forward(nf, fetched)

            @pl.when(op == 1)
            def _():
                do_backward(nb, nf, fetched)

            @pl.when(op == 2)
            def _():
                do_weights(nw)

            if CODES_H or CODES_G:
                @pl.when(op == 3)
                def _():
                    do_relay(nr)

            late = jnp.maximum(nb - (micro - LATE) * PIECES, 0)
            m = jnp.where(late > 0, micro - LATE + lax.div(late, FINE), lax.div(nb, PIECES))
            more = jnp.where((m + 1 < micro) & (nf >= steps_before(m + 2)), m + 2, m + 1)
            begins = jnp.where(late > 0, lax.rem(late, FINE), lax.rem(nb, PIECES)) == 0
            fetched = jnp.where((op == 1) & begins, more, fetched)
            one = jnp.int32(1)
            return (lax.div(word, 4), nf + jnp.where(op == 0, one, 0), nb + jnp.where(op == 1, one, 0),
                    nw + jnp.where(op == 2, one, 0), nr + jnp.where(op == 3, one, 0), fetched)

        return lax.fori_loop(0, jnp.minimum(15, total - 15 * w), turn, (word, *carry))[1:]

    lax.fori_loop(0, lax.div(total + 14, 15), block, (jnp.int32(0),) * 5)

    wg[...] = acc_g[...].astype(bf16)
    outs = [pltpu.make_async_copy(b, a.at[0], o_sem.at[i]) for i, (a, b) in enumerate(((og, wg), (ou, wu), (od, wd)))]
    outs[0].start()
    wu[...] = acc_u[...].astype(bf16)
    outs[1].start()
    wd[...] = acc_d[...].astype(bf16).T
    outs[2].start()

    @pl.when(me < stages - 1)
    def _():
        for m in range(micro - OUTS, micro):
            sent_h(m)

    @pl.when(me > 0)
    def _():
        for m in range(micro):
            remote(g_v.at[m], g_v.at[m], gs_sem.at[m], g_sem.at[m, 0], me - 1).wait_send()

    for via, codes in ((VIA_H, CODES_H), (VIA_G, CODES_G)):
        @pl.when(me == via)
        def _():
            for c in codes:
                remote(relay.at[c], relay.at[c], rs_sem.at[c], rr_sem.at[c], TURN_H).wait_send()

    for out in outs:
        out.wait()


def settle(a, b, c, oa, ob, oc, va, vb, vc, in_sem, out_sem):
    todo = []
    for i, (src, via, dst) in enumerate(((a, va, oa), (b, vb, ob), (c, vc, oc))):
        half = src.shape[1] // 2
        for p in range(2):
            at = pl.ds(p * half, half)
            todo.append((pltpu.make_async_copy(src.at[0, at], via.at[at], in_sem.at[i, p]), pltpu.make_async_copy(via.at[at], dst.at[0, at], out_sem.at[i, p])))
    for load, _ in todo:
        load.start()
    for load, store in todo:
        load.wait()
        store.start()
    for _, store in todo:
        store.wait()


def solution(mesh):
    stages = mesh.shape["pp"]

    def step(x, dy, w_gate, w_up, w_down):
        micro, rows, d = x.shape
        ff = w_gate.shape[2]
        hbm, vmem, dma = pl.BlockSpec(memory_space=pl.ANY), pltpu.VMEM, pltpu.SemaphoreType.DMA
        outs = pl.pallas_call(
            functools.partial(kernel, stages),
            out_shape=(
                jax.ShapeDtypeStruct(w_gate.shape, bf16),
                jax.ShapeDtypeStruct(w_up.shape, bf16),
                jax.ShapeDtypeStruct(w_down.shape, bf16),
                jax.ShapeDtypeStruct((micro, rows, ff), f32),
                jax.ShapeDtypeStruct((micro, rows, ff), f32),
                jax.ShapeDtypeStruct((micro, rows, ff), bf16),
                jax.ShapeDtypeStruct((micro * PIECES, rows // PIECES, d), bf16),
            ),
            in_specs=[hbm] * 5,
            out_specs=(hbm,) * 7,
            scratch_shapes=[
                vmem((d, ff), bf16), vmem((d, ff), bf16), vmem((ff, d), bf16),
                vmem((ff, d), bf16), vmem((ff, d), bf16), vmem((d, ff), bf16),
                vmem((d, ff), f32), vmem((d, ff), f32), vmem((d, ff), f32),
                vmem((micro, rows, d), bf16), vmem((micro, rows, d), bf16), vmem((OUTS, rows, d), bf16),
                vmem((SLOTS, rows, ff), f32), vmem((SLOTS, rows, ff), f32), vmem((SLOTS, rows, ff), bf16),
                vmem((rows, ff), bf16), vmem((rows, ff), bf16), vmem((d, rows), bf16), vmem((d, rows), bf16),
                dma((3,)), dma((micro, FINE)), dma((micro, FINE)), dma((OUTS,)), dma((micro,)), dma((PIECES, 3)), dma((2, 3)), dma((3,)),
                dma((micro * PIECES,)), dma((micro * PIECES,)),
            ],
            compiler_params=pltpu.CompilerParams(collective_id=0, has_side_effects=True, vmem_limit_bytes=67043328),
        )(x, dy, w_gate, w_up, w_down)
        shapes = [jax.ShapeDtypeStruct(o.shape, bf16) for o in outs[:3]]
        return pl.pallas_call(
            settle,
            out_shape=shapes,
            in_specs=[hbm] * 3,
            out_specs=[hbm] * 3,
            scratch_shapes=[vmem(o.shape[1:], bf16) for o in shapes] + [dma((3, 2)), dma((3, 2))],
        )(*outs[:3])

    return jax.shard_map(
        step,
        mesh=mesh,
        in_specs=(P("rep", None, None),) * 2 + (P("pp", None, None),) * 3,
        out_specs=(P(("rep", "pp"), None, None),) * 3,
        check_vma=False,
    )
```

```python
import functools

import jax
import jax.numpy as jnp
from jax import lax
from jax.experimental import pallas as pl
from jax.experimental.pallas import tpu as pltpu
from jax.sharding import PartitionSpec as P

f32, bf16 = jnp.float32, jnp.bfloat16
SLOTS = 3
OUTS = 3
PIECES = 2
FINE = 4
EARLY, LATE = 4, 4
TURN_H, VIA_H, TURN_G, VIA_G = 3, 0, 4, 7
CODES_H = (8, 10, 11, 12, 14, 16, 17, 18, 19, 21, 22, 23, 25, 26, 27, 29, 31)
CODES_G = (0, 1, 5, 8, 13, 17)
LENGTHS = [113, 96, 96, 96, 96, 96, 96, 102]
TABLE = (
    (0, 0, 125828144, 813052280, 912160662, 630610777, 374707557, 38245),
    (0, 0, 26240256, 374956313, 374957462, 358963542, 2390, 0),
    (0, 557842432, 610341009, 555238932, 374957457, 358963542, 2390, 0),
    (0, 407109632, 152584484, 105156997, 374957156, 358963542, 2390, 0),
    (0, 100734996, 76842369, 345375073, 92561688, 358963542, 2390, 0),
    (0, 68293012, 610361366, 629168145, 542708292, 358963285, 2390, 0),
    (537198592, 21585925, 92364882, 86005848, 360732760, 357045601, 2390, 0),
    (23069952, 629345632, 369576016, 815040352, 567809157, 139821396, 9789525, 0),
)
TILE = 256


def dot(a, b):
    return jnp.dot(a, b, preferred_element_type=f32)


def normed(h):
    wide = h.astype(f32)
    scale = lax.rsqrt(jnp.mean(wide * wide, -1, keepdims=True) + 1e-6)
    return wide, scale


def forward(h_ref, wg, wu, wd, si_ref, m_ref, hid_ref, out_ref):
    wide, scale = normed(h_ref[...])
    a = (wide * scale).astype(bf16)
    for j in range(wg.shape[1] // TILE):
        cs = pl.ds(j * TILE, TILE)
        g, u = dot(a, wg[:, cs]), dot(a, wu[:, cs])
        s = 1.0 / (1.0 + jnp.exp(-g))
        si = g * s
        si_ref[:, cs] = si
        m_ref[:, cs] = u * (s + si * (1.0 - s))
        hid_ref[:, cs] = (si * u).astype(bf16)
    if out_ref is not None:
        for j in range(wd.shape[1] // TILE):
            cs = pl.ds(j * TILE, TILE)
            out_ref[:, cs] = h_ref[:, cs] + dot(hid_ref[...], wd[:, cs]).astype(bf16)


def backward(h_ref, dy_ref, wgt, wut, wdt, si_ref, m_ref, dg_ref, du_ref, at_ref, gt_ref, through):
    dy = dy_ref[...]
    for j in range(wdt.shape[1] // TILE):
        cs = pl.ds(j * TILE, TILE)
        dh = dot(dy, wdt[:, cs]).astype(bf16).astype(f32)
        dg_ref[:, cs] = (dh * m_ref[:, cs]).astype(bf16)
        du_ref[:, cs] = (dh * si_ref[:, cs]).astype(bf16)
    wide, scale = normed(h_ref[...])
    at_ref[...] = (wide * scale).astype(bf16).T
    gt_ref[...] = dy.T
    if through:
        da = dot(dg_ref[...], wgt[...]).astype(bf16) + dot(du_ref[...], wut[...]).astype(bf16)
        da = da.astype(f32)
        c = jnp.mean(da * wide, -1, keepdims=True) * (scale * scale)
        dy_ref[...] = dy + (scale * (da - wide * c)).astype(bf16)


def weights_term(acc, left, right):
    for j in range(right.shape[1] // TILE):
        cs = pl.ds(j * TILE, TILE)
        acc[:, cs] += dot(left[...], right[:, cs]).astype(bf16).astype(f32)


def pick(index, values):
    out = values[-1]
    for i in range(len(values) - 2, -1, -1):
        out = jnp.where(index == i, values[i], out)
    return jnp.int32(out)


def kernel(stages, x, dy, wg_h, wu_h, wd_h, og, ou, od, si_h, m_h, hid_h, relay,
           wg, wu, wd, wgt, wut, wdt, acc_g, acc_u, acc_d, h_v, g_v, h_out, si_v, m_v, hid_v, dg_v, du_v, at_v, gt_v,
           w_sem, h_sem, g_sem, hs_sem, gs_sem, out_sem, in_sem, o_sem, rr_sem, rs_sem):
    me = lax.axis_index("pp")
    micro, rows = x.shape[0], x.shape[1]
    size = rows // PIECES
    first, last = me == 0, me == stages - 1
    spill = me < stages - 2

    barrier = pltpu.get_barrier_semaphore()
    for peer in range(stages - 1):
        to = lax.rem(me + peer + 1, stages)
        pl.semaphore_signal(barrier, inc=1, device_id={"pp": to}, device_id_type=pl.DeviceIdType.MESH)

    loads = [pltpu.make_async_copy(a.at[0], b, w_sem.at[i]) for i, (a, b) in enumerate(((wg_h, wg), (wu_h, wu), (wd_h, wd)))]

    def load_pieces(m, src, to, sem, count=PIECES):
        for p in range(count):
            at = pl.ds(p * (rows // count), rows // count)
            pltpu.make_async_copy(src.at[m, at], to.at[m, at], sem.at[m, p]).start()

    @pl.when(first)
    def _():
        load_pieces(0, x, h_v, h_sem, FINE)

    for load in loads:
        load.start()

    @pl.when(first)
    def _():
        for m in range(1, EARLY):
            load_pieces(m, x, h_v, h_sem, FINE)

        @pl.loop(EARLY, micro)
        def _(m):
            load_pieces(m, x, h_v, h_sem)

    @pl.when(last)
    def _():
        @pl.loop(0, micro - LATE)
        def _(m):
            load_pieces(m, dy, g_v, g_sem)

        for m in range(micro - LATE, micro):
            load_pieces(m, dy, g_v, g_sem, FINE)

    for acc in (acc_g, acc_u, acc_d):
        acc[...] = jnp.zeros_like(acc)
    for load in loads:
        load.wait()
    pl.semaphore_wait(barrier, stages - 1)

    @pl.when(me > 0)
    def _():
        wgt[...] = wg[...].T
        wut[...] = wu[...].T
        wdt[...] = wd[...].T

    def arrived(buf, sem, m, p, at):
        pltpu.make_async_copy(buf.at[m, at], buf.at[m, at], sem.at[m, p]).wait()

    def remote(src, dst, send, recv, to):
        return pltpu.make_async_remote_copy(src, dst, send, recv, device_id={"pp": to}, device_id_type=pl.DeviceIdType.MESH)

    def relayed(codes, m, p):
        low, high = (sum(1 << c % 16 for c in codes if c // 16 == part) for part in range(2))
        code = m * PIECES + p
        word = jnp.where(code < 16, low, high)
        return lax.rem(lax.shift_right_logical(jnp.int32(word), lax.rem(code, 16)), 2) == 1

    def pass_on(src, m, p, at, send, dst, recv, to, turn, via, codes):
        detour = (me == turn) & relayed(codes, m, p) if codes else False

        @pl.when(jnp.logical_not(detour))
        def _():
            remote(src, dst.at[m, at], send, recv.at[m, p], to).start()

        if codes:
            @pl.when(detour)
            def _():
                remote(src, relay.at[m * PIECES + p], send, rr_sem.at[m * PIECES + p], via).start()

    def sent_h(m):
        o = lax.rem(m, OUTS)
        remote(h_out.at[o], h_v.at[m], hs_sem.at[o], h_sem.at[m, 0], me + 1).wait_send()

    outs = [pltpu.make_async_copy(b, a.at[0], o_sem.at[i]) for i, (a, b) in enumerate(((og, wg), (ou, wu), (od, wd)))]
    saved = ((si_v, si_h), (m_v, m_h), (hid_v, hid_h))

    def spill_out(m, p, at):
        return [pltpu.make_async_copy(v.at[0, at], h.at[m, at], out_sem.at[p, i]) for i, (v, h) in enumerate(saved)]

    def spill_in(m):
        slot = lax.rem(m, 2)
        return [pltpu.make_async_copy(h.at[m], v.at[1 + slot], in_sem.at[slot, i]) for i, (v, h) in enumerate(saved)]

    def rows_of(p, size=size):
        return pl.ds(pl.multiple_of(p * size, size), size)

    finer = FINE // PIECES

    def steps_before(m):
        return m * PIECES + jnp.minimum(m, EARLY) * (FINE - PIECES)

    def do_forward(n, fetched):
        fine = n < FINE * EARLY
        coarse = jnp.maximum(n - FINE * EARLY, 0)
        m = jnp.where(fine, lax.div(n, FINE), EARLY + lax.div(coarse, PIECES))
        p = jnp.where(fine, lax.rem(n, FINE), lax.rem(coarse, PIECES))
        half = jnp.where(fine, lax.div(p, finer), p)
        opens = jnp.logical_not(fine) | (lax.rem(p, finer) == 0)
        closes = jnp.logical_not(fine) | (lax.rem(p, finer) == finer - 1)
        slot = jnp.where(spill, 0, lax.rem(m, SLOTS))
        o = lax.rem(m, OUTS)

        @pl.when(spill & opens & (m > 0) & (fetched < m))
        def _():
            for copy in spill_out(m - 1, half, rows_of(half)):
                copy.wait()

        @pl.when((p == 0) & (m >= OUTS) & (me < stages - 1))
        def _():
            sent_h(m - OUTS)

        def work(size, codes):
            at = rows_of(p, size)
            arrived(h_v, h_sem, m, p, at)
            keep = si_v.at[slot, at], m_v.at[slot, at], hid_v.at[slot, at]

            @pl.when(me < stages - 1)
            def _():
                forward(h_v.at[m, at], wg, wu, wd, *keep, h_out.at[o, at])
                pass_on(h_out.at[o, at], m, p, at, hs_sem.at[o], h_v, h_sem, me + 1, TURN_H, VIA_H, codes)

            @pl.when(last)
            def _():
                forward(h_v.at[m, at], wg, wu, wd, *keep, None)

        @pl.when(fine)
        def _():
            work(rows // FINE, ())

        @pl.when(jnp.logical_not(fine))
        def _():
            work(size, CODES_H)

        @pl.when(spill & closes)
        def _():
            for copy in spill_out(m, half, rows_of(half)):
                copy.start()

    def fetch(m, forwards):
        for p in range(PIECES):
            @pl.when(forwards <= steps_before(m + 1) + p * jnp.where(m + 1 < EARLY, finer, 1))
            def _():
                for copy in spill_out(m, p, pl.ds(p * size, size)):
                    copy.wait()

        for copy in spill_in(m):
            copy.start()

    def do_backward(n, forwards, fetched):
        fine = n >= (micro - LATE) * PIECES
        late = jnp.maximum(n - (micro - LATE) * PIECES, 0)
        m = jnp.where(fine, micro - LATE + lax.div(late, FINE), lax.div(n, PIECES))
        p = jnp.where(fine, lax.rem(late, FINE), lax.rem(n, PIECES))
        slot = jnp.where(spill, 1 + lax.rem(m, 2), lax.rem(m, SLOTS))

        @pl.when(first & (n == 0))
        def _():
            wdt[...] = wd[...].T

        @pl.when(spill & (p == 0))
        def _():
            @pl.when(fetched <= m)
            def _():
                fetch(m, forwards)

            for copy in spill_in(m):
                copy.wait()

            @pl.when((m + 1 < micro) & (forwards >= steps_before(m + 2)))
            def _():
                fetch(m + 1, forwards)

        def work(size, codes):
            at = rows_of(p, size)
            arrived(g_v, g_sem, m, p, at)

            def piece(through):
                backward(h_v.at[m, at], g_v.at[m, at], wgt, wut, wdt, si_v.at[slot, at], m_v.at[slot, at],
                         dg_v.at[at], du_v.at[at], at_v.at[:, at], gt_v.at[:, at], through)

            @pl.when(me > 0)
            def _():
                piece(True)
                pass_on(g_v.at[m, at], m, p, at, gs_sem.at[m], g_v, g_sem, me - 1, TURN_G, VIA_G, codes)

            @pl.when(first)
            def _():
                piece(False)

        @pl.when(fine)
        def _():
            work(rows // FINE, ())

        @pl.when(jnp.logical_not(fine))
        def _():
            work(size, CODES_G)

    def do_weights(m):
        slot = jnp.where(spill, 1 + lax.rem(m, 2), lax.rem(m, SLOTS))
        terms = (acc_g, at_v, dg_v), (acc_u, at_v, du_v), (acc_d, gt_v, hid_v.at[slot])

        @pl.when(m < micro - 1)
        def _():
            for term in terms:
                weights_term(*term)

        @pl.when(m == micro - 1)
        def _():
            for i, (term, w, out) in enumerate(zip(terms, (wg, wu, wd), outs, strict=True)):
                weights_term(*term)
                total = term[0][...].astype(bf16)
                w[...] = total.T if i == 2 else total
                out.start()

    def do_relay(n):
        def hop(codes, dst, recv, to):
            c = pick(n, codes)
            m, p = lax.div(c, PIECES), lax.rem(c, PIECES)
            pltpu.make_async_copy(relay.at[c], relay.at[c], rr_sem.at[c]).wait()
            remote(relay.at[c], dst.at[m, rows_of(p)], rs_sem.at[c], recv.at[m, p], to).start()

        if CODES_H:
            @pl.when(me == VIA_H)
            def _():
                hop(CODES_H, h_v, h_sem, TURN_H + 1)

        if CODES_G:
            @pl.when(me == VIA_G)
            def _():
                hop(CODES_G, g_v, g_sem, TURN_G - 1)

    total = pick(me, LENGTHS)
    words = len(TABLE[0])

    def block(w, carry):
        word = pick(w, [pick(me, [row[i] for row in TABLE]) for i in range(words)])

        def turn(_, carry):
            word, nf, nb, nw, nr, fetched = carry
            op = lax.rem(word, 4)

            @pl.when(op == 0)
            def _():
                do_forward(nf, fetched)

            @pl.when(op == 1)
            def _():
                do_backward(nb, nf, fetched)

            @pl.when(op == 2)
            def _():
                do_weights(nw)

            if CODES_H or CODES_G:
                @pl.when(op == 3)
                def _():
                    do_relay(nr)

            late = jnp.maximum(nb - (micro - LATE) * PIECES, 0)
            m = jnp.where(late > 0, micro - LATE + lax.div(late, FINE), lax.div(nb, PIECES))
            more = jnp.where((m + 1 < micro) & (nf >= steps_before(m + 2)), m + 2, m + 1)
            begins = jnp.where(late > 0, lax.rem(late, FINE), lax.rem(nb, PIECES)) == 0
            fetched = jnp.where((op == 1) & begins, more, fetched)
            one = jnp.int32(1)
            return (lax.div(word, 4), nf + jnp.where(op == 0, one, 0), nb + jnp.where(op == 1, one, 0),
                    nw + jnp.where(op == 2, one, 0), nr + jnp.where(op == 3, one, 0), fetched)

        return lax.fori_loop(0, jnp.minimum(15, total - 15 * w), turn, (word, *carry))[1:]

    lax.fori_loop(0, lax.div(total + 14, 15), block, (jnp.int32(0),) * 5)

    @pl.when(me < stages - 1)
    def _():
        for m in range(micro - OUTS, micro):
            sent_h(m)

    @pl.when(me > 0)
    def _():
        for m in range(micro):
            remote(g_v.at[m], g_v.at[m], gs_sem.at[m], g_sem.at[m, 0], me - 1).wait_send()

    for via, codes in ((VIA_H, CODES_H), (VIA_G, CODES_G)):
        @pl.when(me == via)
        def _():
            for c in codes:
                remote(relay.at[c], relay.at[c], rs_sem.at[c], rr_sem.at[c], TURN_H).wait_send()

    for out in outs:
        out.wait()


def settle(a, b, c, oa, ob, oc, va, vb, vc, in_sem, out_sem):
    todo = []
    for i, (src, via, dst) in enumerate(((a, va, oa), (b, vb, ob), (c, vc, oc))):
        half = src.shape[1] // 2
        for p in range(2):
            at = pl.ds(p * half, half)
            todo.append((pltpu.make_async_copy(src.at[0, at], via.at[at], in_sem.at[i, p]), pltpu.make_async_copy(via.at[at], dst.at[0, at], out_sem.at[i, p])))
    for load, _ in todo:
        load.start()
    for load, store in todo:
        load.wait()
        store.start()
    for _, store in todo:
        store.wait()


def solution(mesh):
    stages = mesh.shape["pp"]

    def step(x, dy, w_gate, w_up, w_down):
        micro, rows, d = x.shape
        ff = w_gate.shape[2]
        hbm, vmem, dma = pl.BlockSpec(memory_space=pl.ANY), pltpu.VMEM, pltpu.SemaphoreType.DMA
        outs = pl.pallas_call(
            functools.partial(kernel, stages),
            out_shape=(
                jax.ShapeDtypeStruct(w_gate.shape, bf16),
                jax.ShapeDtypeStruct(w_up.shape, bf16),
                jax.ShapeDtypeStruct(w_down.shape, bf16),
                jax.ShapeDtypeStruct((micro, rows, ff), f32),
                jax.ShapeDtypeStruct((micro, rows, ff), f32),
                jax.ShapeDtypeStruct((micro, rows, ff), bf16),
                jax.ShapeDtypeStruct((micro * PIECES, rows // PIECES, d), bf16),
            ),
            in_specs=[hbm] * 5,
            out_specs=(hbm,) * 7,
            scratch_shapes=[
                vmem((d, ff), bf16), vmem((d, ff), bf16), vmem((ff, d), bf16),
                vmem((ff, d), bf16), vmem((ff, d), bf16), vmem((d, ff), bf16),
                vmem((d, ff), f32), vmem((d, ff), f32), vmem((d, ff), f32),
                vmem((micro, rows, d), bf16), vmem((micro, rows, d), bf16), vmem((OUTS, rows, d), bf16),
                vmem((SLOTS, rows, ff), f32), vmem((SLOTS, rows, ff), f32), vmem((SLOTS, rows, ff), bf16),
                vmem((rows, ff), bf16), vmem((rows, ff), bf16), vmem((d, rows), bf16), vmem((d, rows), bf16),
                dma((3,)), dma((micro, FINE)), dma((micro, FINE)), dma((OUTS,)), dma((micro,)), dma((PIECES, 3)), dma((2, 3)), dma((3,)),
                dma((micro * PIECES,)), dma((micro * PIECES,)),
            ],
            compiler_params=pltpu.CompilerParams(collective_id=0, has_side_effects=True, vmem_limit_bytes=67043328),
        )(x, dy, w_gate, w_up, w_down)
        shapes = [jax.ShapeDtypeStruct(o.shape, bf16) for o in outs[:3]]
        return pl.pallas_call(
            settle,
            out_shape=shapes,
            in_specs=[hbm] * 3,
            out_specs=[hbm] * 3,
            scratch_shapes=[vmem(o.shape[1:], bf16) for o in shapes] + [dma((3, 2)), dma((3, 2))],
        )(*outs[:3])

    return jax.shard_map(
        step,
        mesh=mesh,
        in_specs=(P("rep", None, None),) * 2 + (P("pp", None, None),) * 3,
        out_specs=(P(("rep", "pp"), None, None),) * 3,
        check_vma=False,
    )
```

```python
import functools

import jax
import jax.numpy as jnp
from jax import lax
from jax.experimental import pallas as pl
from jax.experimental.pallas import tpu as pltpu
from jax.sharding import PartitionSpec as P

f32, bf16 = jnp.float32, jnp.bfloat16
SLOTS = 3
OUTS = 3
PIECES = 2
FINE = 4
EARLY, LATE = 4, 4
TURN_H, VIA_H, TURN_G, VIA_G = 3, 0, 4, 7
CODES_H = (8, 10, 11, 12, 14, 16, 17, 18, 19, 21, 22, 23, 25, 26, 27, 29, 31)
CODES_G = (0, 1, 5, 8, 13, 17)
LENGTHS = [113, 96, 96, 96, 96, 96, 96, 102]
TABLE = (
    (0, 0, 125828144, 813052280, 912160662, 630610777, 374707557, 38245),
    (0, 0, 26240256, 374956313, 374957462, 358963542, 2390, 0),
    (0, 557842432, 610341009, 555238932, 374957457, 358963542, 2390, 0),
    (0, 407109632, 152584484, 105156997, 374957156, 358963542, 2390, 0),
    (0, 100734996, 76842369, 345375073, 92561688, 358963542, 2390, 0),
    (0, 68293012, 610361366, 629168145, 542708292, 358963285, 2390, 0),
    (537198592, 21585925, 92364882, 86005848, 360732760, 357045601, 2390, 0),
    (23069952, 629345632, 369576016, 815040352, 567809157, 139821396, 9789525, 0),
)
TILE = 256


def dot(a, b):
    return jnp.dot(a, b, preferred_element_type=f32)


def normed(h):
    wide = h.astype(f32)
    scale = lax.rsqrt(jnp.mean(wide * wide, -1, keepdims=True) + 1e-6)
    return wide, scale


def forward(h_ref, wg, wu, wd, si_ref, m_ref, hid_ref, out_ref):
    wide, scale = normed(h_ref[...])
    a = (wide * scale).astype(bf16)
    for j in range(wg.shape[1] // TILE):
        cs = pl.ds(j * TILE, TILE)
        g, u = dot(a, wg[:, cs]), dot(a, wu[:, cs])
        s = 1.0 / (1.0 + jnp.exp(-g))
        si = g * s
        si_ref[:, cs] = si
        m_ref[:, cs] = u * (s + si * (1.0 - s))
        hid_ref[:, cs] = (si * u).astype(bf16)
    if out_ref is not None:
        for j in range(wd.shape[1] // TILE):
            cs = pl.ds(j * TILE, TILE)
            out_ref[:, cs] = h_ref[:, cs] + dot(hid_ref[...], wd[:, cs]).astype(bf16)


def backward(h_ref, dy_ref, wgt, wut, wdt, si_ref, m_ref, dg_ref, du_ref, at_ref, gt_ref, through):
    dy = dy_ref[...]
    for j in range(wdt.shape[1] // TILE):
        cs = pl.ds(j * TILE, TILE)
        dh = dot(dy, wdt[:, cs]).astype(bf16).astype(f32)
        dg_ref[:, cs] = (dh * m_ref[:, cs]).astype(bf16)
        du_ref[:, cs] = (dh * si_ref[:, cs]).astype(bf16)
    wide, scale = normed(h_ref[...])
    at_ref[...] = (wide * scale).astype(bf16).T
    gt_ref[...] = dy.T
    if through:
        da = dot(dg_ref[...], wgt[...]).astype(bf16) + dot(du_ref[...], wut[...]).astype(bf16)
        da = da.astype(f32)
        c = jnp.mean(da * wide, -1, keepdims=True) * (scale * scale)
        dy_ref[...] = dy + (scale * (da - wide * c)).astype(bf16)


def weights_term(acc, left, right):
    for j in range(right.shape[1] // TILE):
        cs = pl.ds(j * TILE, TILE)
        acc[:, cs] += dot(left[...], right[:, cs]).astype(bf16).astype(f32)


def pick(index, values):
    out = values[-1]
    for i in range(len(values) - 2, -1, -1):
        out = jnp.where(index == i, values[i], out)
    return jnp.int32(out)


def kernel(stages, x, dy, wg_h, wu_h, wd_h, og, ou, od, si_h, m_h, hid_h, relay,
           wg, wu, wd, wgt, wut, wdt, acc_g, acc_u, acc_d, h_v, g_v, h_out, si_v, m_v, hid_v, dg_v, du_v, at_v, gt_v,
           w_sem, h_sem, g_sem, hs_sem, gs_sem, out_sem, in_sem, o_sem, rr_sem, rs_sem):
    me = lax.axis_index("pp")
    micro, rows = x.shape[0], x.shape[1]
    size = rows // PIECES
    first, last = me == 0, me == stages - 1
    spill = me < stages - 2

    barrier = pltpu.get_barrier_semaphore()
    for peer in range(stages - 1):
        to = lax.rem(me + peer + 1, stages)
        pl.semaphore_signal(barrier, inc=1, device_id={"pp": to}, device_id_type=pl.DeviceIdType.MESH)

    loads = [pltpu.make_async_copy(a.at[0], b, w_sem.at[i]) for i, (a, b) in enumerate(((wg_h, wg), (wu_h, wu), (wd_h, wd)))]

    def load_pieces(m, src, to, sem, count=PIECES):
        for p in range(count):
            at = pl.ds(p * (rows // count), rows // count)
            pltpu.make_async_copy(src.at[m, at], to.at[m, at], sem.at[m, p]).start()

    @pl.when(first)
    def _():
        load_pieces(0, x, h_v, h_sem, FINE)

    for load in loads:
        load.start()

    @pl.when(last)
    def _():
        @pl.loop(0, micro - LATE)
        def _(m):
            load_pieces(m, dy, g_v, g_sem)

        for m in range(micro - LATE, micro):
            load_pieces(m, dy, g_v, g_sem, FINE)

    for acc in (acc_g, acc_u, acc_d):
        acc[...] = jnp.zeros_like(acc)
    for load in loads:
        load.wait()
    pl.semaphore_wait(barrier, stages - 1)

    @pl.when(first)
    def _():
        for m in range(1, EARLY):
            load_pieces(m, x, h_v, h_sem, FINE)

        @pl.loop(EARLY, micro)
        def _(m):
            load_pieces(m, x, h_v, h_sem)

    @pl.when(me > 1)
    def _():
        wgt[...] = wg[...].T
        wut[...] = wu[...].T
        wdt[...] = wd[...].T

    def arrived(buf, sem, m, p, at):
        pltpu.make_async_copy(buf.at[m, at], buf.at[m, at], sem.at[m, p]).wait()

    def remote(src, dst, send, recv, to):
        return pltpu.make_async_remote_copy(src, dst, send, recv, device_id={"pp": to}, device_id_type=pl.DeviceIdType.MESH)

    def relayed(codes, m, p):
        low, high = (sum(1 << c % 16 for c in codes if c // 16 == part) for part in range(2))
        code = m * PIECES + p
        word = jnp.where(code < 16, low, high)
        return lax.rem(lax.shift_right_logical(jnp.int32(word), lax.rem(code, 16)), 2) == 1

    def pass_on(src, m, p, at, send, dst, recv, to, turn, via, codes):
        detour = (me == turn) & relayed(codes, m, p) if codes else False

        @pl.when(jnp.logical_not(detour))
        def _():
            remote(src, dst.at[m, at], send, recv.at[m, p], to).start()

        if codes:
            @pl.when(detour)
            def _():
                remote(src, relay.at[m * PIECES + p], send, rr_sem.at[m * PIECES + p], via).start()

    def sent_h(m):
        o = lax.rem(m, OUTS)
        remote(h_out.at[o], h_v.at[m], hs_sem.at[o], h_sem.at[m, 0], me + 1).wait_send()

    outs = [pltpu.make_async_copy(b, a.at[0], o_sem.at[i]) for i, (a, b) in enumerate(((og, wg), (ou, wu), (od, wd)))]
    saved = ((si_v, si_h), (m_v, m_h), (hid_v, hid_h))

    def spill_out(m, p, at):
        return [pltpu.make_async_copy(v.at[0, at], h.at[m, at], out_sem.at[p, i]) for i, (v, h) in enumerate(saved)]

    def spill_in(m):
        slot = lax.rem(m, 2)
        return [pltpu.make_async_copy(h.at[m], v.at[1 + slot], in_sem.at[slot, i]) for i, (v, h) in enumerate(saved)]

    def rows_of(p, size=size):
        return pl.ds(pl.multiple_of(p * size, size), size)

    finer = FINE // PIECES

    def steps_before(m):
        return m * PIECES + jnp.minimum(m, EARLY) * (FINE - PIECES)

    def do_forward(n, fetched):
        fine = n < FINE * EARLY
        coarse = jnp.maximum(n - FINE * EARLY, 0)
        m = jnp.where(fine, lax.div(n, FINE), EARLY + lax.div(coarse, PIECES))
        p = jnp.where(fine, lax.rem(n, FINE), lax.rem(coarse, PIECES))
        half = jnp.where(fine, lax.div(p, finer), p)
        opens = jnp.logical_not(fine) | (lax.rem(p, finer) == 0)
        closes = jnp.logical_not(fine) | (lax.rem(p, finer) == finer - 1)
        slot = jnp.where(spill, 0, lax.rem(m, SLOTS))
        o = lax.rem(m, OUTS)

        @pl.when(spill & opens & (m > 0) & (fetched < m))
        def _():
            for copy in spill_out(m - 1, half, rows_of(half)):
                copy.wait()

        @pl.when((p == 0) & (m >= OUTS) & (me < stages - 1))
        def _():
            sent_h(m - OUTS)

        def work(size, codes):
            at = rows_of(p, size)
            arrived(h_v, h_sem, m, p, at)
            keep = si_v.at[slot, at], m_v.at[slot, at], hid_v.at[slot, at]

            @pl.when(me < stages - 1)
            def _():
                forward(h_v.at[m, at], wg, wu, wd, *keep, h_out.at[o, at])
                pass_on(h_out.at[o, at], m, p, at, hs_sem.at[o], h_v, h_sem, me + 1, TURN_H, VIA_H, codes)

            @pl.when(last)
            def _():
                forward(h_v.at[m, at], wg, wu, wd, *keep, None)

        @pl.when(fine)
        def _():
            work(rows // FINE, ())

        @pl.when(jnp.logical_not(fine))
        def _():
            work(size, CODES_H)

        @pl.when(spill & closes)
        def _():
            for copy in spill_out(m, half, rows_of(half)):
                copy.start()

    def fetch(m, forwards):
        for p in range(PIECES):
            @pl.when(forwards <= steps_before(m + 1) + p * jnp.where(m + 1 < EARLY, finer, 1))
            def _():
                for copy in spill_out(m, p, pl.ds(p * size, size)):
                    copy.wait()

        for copy in spill_in(m):
            copy.start()

    def do_backward(n, forwards, fetched):
        fine = n >= (micro - LATE) * PIECES
        late = jnp.maximum(n - (micro - LATE) * PIECES, 0)
        m = jnp.where(fine, micro - LATE + lax.div(late, FINE), lax.div(n, PIECES))
        p = jnp.where(fine, lax.rem(late, FINE), lax.rem(n, PIECES))
        slot = jnp.where(spill, 1 + lax.rem(m, 2), lax.rem(m, SLOTS))

        @pl.when((me <= 1) & (n == 0))
        def _():
            wgt[...] = wg[...].T
            wut[...] = wu[...].T
            wdt[...] = wd[...].T

        @pl.when(spill & (p == 0))
        def _():
            @pl.when(fetched <= m)
            def _():
                fetch(m, forwards)

            for copy in spill_in(m):
                copy.wait()

            @pl.when((m + 1 < micro) & (forwards >= steps_before(m + 2)))
            def _():
                fetch(m + 1, forwards)

        def work(size, codes):
            at = rows_of(p, size)
            arrived(g_v, g_sem, m, p, at)

            def piece(through):
                backward(h_v.at[m, at], g_v.at[m, at], wgt, wut, wdt, si_v.at[slot, at], m_v.at[slot, at],
                         dg_v.at[at], du_v.at[at], at_v.at[:, at], gt_v.at[:, at], through)

            @pl.when(me > 0)
            def _():
                piece(True)
                pass_on(g_v.at[m, at], m, p, at, gs_sem.at[m], g_v, g_sem, me - 1, TURN_G, VIA_G, codes)

            @pl.when(first)
            def _():
                piece(False)

        @pl.when(fine)
        def _():
            work(rows // FINE, ())

        @pl.when(jnp.logical_not(fine))
        def _():
            work(size, CODES_G)

    def do_weights(m):
        slot = jnp.where(spill, 1 + lax.rem(m, 2), lax.rem(m, SLOTS))
        terms = (acc_g, at_v, dg_v), (acc_u, at_v, du_v), (acc_d, gt_v, hid_v.at[slot])

        @pl.when(m < micro - 1)
        def _():
            for term in terms:
                weights_term(*term)

        @pl.when(m == micro - 1)
        def _():
            for i, (term, w, out) in enumerate(zip(terms, (wg, wu, wd), outs, strict=True)):
                weights_term(*term)
                total = term[0][...].astype(bf16)
                w[...] = total.T if i == 2 else total
                out.start()

    def do_relay(n):
        def hop(codes, dst, recv, to):
            c = pick(n, codes)
            m, p = lax.div(c, PIECES), lax.rem(c, PIECES)
            pltpu.make_async_copy(relay.at[c], relay.at[c], rr_sem.at[c]).wait()
            remote(relay.at[c], dst.at[m, rows_of(p)], rs_sem.at[c], recv.at[m, p], to).start()

        if CODES_H:
            @pl.when(me == VIA_H)
            def _():
                hop(CODES_H, h_v, h_sem, TURN_H + 1)

        if CODES_G:
            @pl.when(me == VIA_G)
            def _():
                hop(CODES_G, g_v, g_sem, TURN_G - 1)

    total = pick(me, LENGTHS)
    words = len(TABLE[0])

    def block(w, carry):
        word = pick(w, [pick(me, [row[i] for row in TABLE]) for i in range(words)])

        def turn(_, carry):
            word, nf, nb, nw, nr, fetched = carry
            op = lax.rem(word, 4)

            @pl.when(op == 0)
            def _():
                do_forward(nf, fetched)

            @pl.when(op == 1)
            def _():
                do_backward(nb, nf, fetched)

            @pl.when(op == 2)
            def _():
                do_weights(nw)

            if CODES_H or CODES_G:
                @pl.when(op == 3)
                def _():
                    do_relay(nr)

            late = jnp.maximum(nb - (micro - LATE) * PIECES, 0)
            m = jnp.where(late > 0, micro - LATE + lax.div(late, FINE), lax.div(nb, PIECES))
            more = jnp.where((m + 1 < micro) & (nf >= steps_before(m + 2)), m + 2, m + 1)
            begins = jnp.where(late > 0, lax.rem(late, FINE), lax.rem(nb, PIECES)) == 0
            fetched = jnp.where((op == 1) & begins, more, fetched)
            one = jnp.int32(1)
            return (lax.div(word, 4), nf + jnp.where(op == 0, one, 0), nb + jnp.where(op == 1, one, 0),
                    nw + jnp.where(op == 2, one, 0), nr + jnp.where(op == 3, one, 0), fetched)

        return lax.fori_loop(0, jnp.minimum(15, total - 15 * w), turn, (word, *carry))[1:]

    lax.fori_loop(0, lax.div(total + 14, 15), block, (jnp.int32(0),) * 5)

    @pl.when(me < stages - 1)
    def _():
        for m in range(micro - OUTS, micro):
            sent_h(m)

    @pl.when(me > 0)
    def _():
        for m in range(micro):
            remote(g_v.at[m], g_v.at[m], gs_sem.at[m], g_sem.at[m, 0], me - 1).wait_send()

    for via, codes in ((VIA_H, CODES_H), (VIA_G, CODES_G)):
        @pl.when(me == via)
        def _():
            for c in codes:
                remote(relay.at[c], relay.at[c], rs_sem.at[c], rr_sem.at[c], TURN_H).wait_send()

    for out in outs:
        out.wait()


def settle(a, b, c, oa, ob, oc, va, vb, vc, in_sem, out_sem):
    todo = []
    for i, (src, via, dst) in enumerate(((a, va, oa), (b, vb, ob), (c, vc, oc))):
        half = src.shape[1] // 2
        for p in range(2):
            at = pl.ds(p * half, half)
            todo.append((pltpu.make_async_copy(src.at[0, at], via.at[at], in_sem.at[i, p]), pltpu.make_async_copy(via.at[at], dst.at[0, at], out_sem.at[i, p])))
    for load, _ in todo:
        load.start()
    for load, store in todo:
        load.wait()
        store.start()
    for _, store in todo:
        store.wait()


def solution(mesh):
    stages = mesh.shape["pp"]

    def step(x, dy, w_gate, w_up, w_down):
        micro, rows, d = x.shape
        ff = w_gate.shape[2]
        hbm, vmem, dma = pl.BlockSpec(memory_space=pl.ANY), pltpu.VMEM, pltpu.SemaphoreType.DMA
        outs = pl.pallas_call(
            functools.partial(kernel, stages),
            out_shape=(
                jax.ShapeDtypeStruct(w_gate.shape, bf16),
                jax.ShapeDtypeStruct(w_up.shape, bf16),
                jax.ShapeDtypeStruct(w_down.shape, bf16),
                jax.ShapeDtypeStruct((micro, rows, ff), f32),
                jax.ShapeDtypeStruct((micro, rows, ff), f32),
                jax.ShapeDtypeStruct((micro, rows, ff), bf16),
                jax.ShapeDtypeStruct((micro * PIECES, rows // PIECES, d), bf16),
            ),
            in_specs=[hbm] * 5,
            out_specs=(hbm,) * 7,
            scratch_shapes=[
                vmem((d, ff), bf16), vmem((d, ff), bf16), vmem((ff, d), bf16),
                vmem((ff, d), bf16), vmem((ff, d), bf16), vmem((d, ff), bf16),
                vmem((d, ff), f32), vmem((d, ff), f32), vmem((d, ff), f32),
                vmem((micro, rows, d), bf16), vmem((micro, rows, d), bf16), vmem((OUTS, rows, d), bf16),
                vmem((SLOTS, rows, ff), f32), vmem((SLOTS, rows, ff), f32), vmem((SLOTS, rows, ff), bf16),
                vmem((rows, ff), bf16), vmem((rows, ff), bf16), vmem((d, rows), bf16), vmem((d, rows), bf16),
                dma((3,)), dma((micro, FINE)), dma((micro, FINE)), dma((OUTS,)), dma((micro,)), dma((PIECES, 3)), dma((2, 3)), dma((3,)),
                dma((micro * PIECES,)), dma((micro * PIECES,)),
            ],
            compiler_params=pltpu.CompilerParams(collective_id=0, has_side_effects=True, vmem_limit_bytes=67043328),
        )(x, dy, w_gate, w_up, w_down)
        shapes = [jax.ShapeDtypeStruct(o.shape, bf16) for o in outs[:3]]
        return pl.pallas_call(
            settle,
            out_shape=shapes,
            in_specs=[hbm] * 3,
            out_specs=[hbm] * 3,
            scratch_shapes=[vmem(o.shape[1:], bf16) for o in shapes] + [dma((3, 2)), dma((3, 2))],
        )(*outs[:3])

    return jax.shard_map(
        step,
        mesh=mesh,
        in_specs=(P("rep", None, None),) * 2 + (P("pp", None, None),) * 3,
        out_specs=(P(("rep", "pp"), None, None),) * 3,
        check_vma=False,
    )
```
